8 devices in a mesh: dp: 2 (over y, z), sp: 4 (over x, core).
Axes of the slice: x: 2, y: 2, z: 1, core: 2. Of those that a mesh axis runs over, the one named last changes fastest.
Arguments:
- x: bfloat16 [4096, 5120], P(('dp', 'sp')), parts along dimension 0
- gain: bfloat16 [5120], replicated
- wq: bfloat16 [5120, 4096], replicated
- wk: bfloat16 [5120, 1024], replicated
- wv: bfloat16 [5120, 1024], replicated
- wo: bfloat16 [4096, 5120], replicated
Outputs:
- output: bfloat16 [4096, 5120], P(('dp', 'sp')), parts along dimension 0
There are 2 independent parts. The reference program is written for one: setup_inputs(seed, part) draws one part's arguments, and reference() takes and returns one part's arrays. A program takes and returns all parts, laid end to end along the dimension named above; an argument that names none is the same for every part.
All inputs are finite; a program needn't handle non-finite values.
Results may differ from the reference program's by a relative error of at most 0.012.
Values are sent between devices in bfloat16 or wider.
A program may use at most 2 GiB of HBM per device.

```python
import jax
import jax.numpy as jnp
from jax import lax

ROWS = 2048
D = 5120
HEADS = 32
KV_HEADS = 8
HEAD = 128
THETA = 10000


def setup_inputs(seed: int = 0, part: int = 0) -> dict:
    kx, kn, kq, kk, kv, ko = jax.random.split(jax.random.key(seed), 6)

    def weights(key, rows, columns):
        return jax.random.normal(key, (rows, columns), jnp.float32) * rows**-0.5

    drawn = {
        "x": jax.random.normal(jax.random.fold_in(kx, part), (ROWS, D), jnp.float32),
        "gain": 1 + 0.1 * jax.random.normal(kn, (D,), jnp.float32),
        "wq": 2 * weights(kq, D, HEADS * HEAD),
        "wk": 2 * weights(kk, D, KV_HEADS * HEAD),
        "wv": 4 * weights(kv, D, KV_HEADS * HEAD),
        "wo": weights(ko, HEADS * HEAD, D),
    }
    return {k: v.astype(jnp.bfloat16) for k, v in drawn.items()}


def normed(x, gain):
    wide = x.astype(jnp.float32)
    scale = lax.rsqrt(jnp.mean(wide * wide, -1, keepdims=True) + 1e-6)
    return (wide * scale * gain.astype(jnp.float32)).astype(jnp.bfloat16)


def turned(t, place, theta):
    half = t.shape[-1] // 2
    angle = place.astype(jnp.float32)[:, None] * theta ** (-jnp.arange(half, dtype=jnp.float32) / half)
    cos, sin = jnp.cos(angle)[:, None], jnp.sin(angle)[:, None]
    a, b = t[..., :half].astype(jnp.float32), t[..., half:].astype(jnp.float32)
    return jnp.concatenate([a * cos - b * sin, b * cos + a * sin], -1).astype(jnp.bfloat16)


def matmul(a, w):
    return jnp.dot(a, w, preferred_element_type=jnp.float32).astype(jnp.bfloat16)


def einsum(form, a, b):
    return jnp.einsum(form, a.astype(jnp.float32), b.astype(jnp.float32))


def attention(q, k, v):
    scores = einsum("tgsd,ugd->gstu", q, k) * q.shape[-1] ** -0.5
    token = jnp.arange(q.shape[0])
    scores = jnp.where(token[:, None] >= token, scores, -jnp.inf)
    weights = jax.nn.softmax(scores, -1).astype(jnp.bfloat16)
    return einsum("gstu,ugd->tgsd", weights, v).astype(jnp.bfloat16)


def reference(x, gain, wq, wk, wv, wo):
    a, place = normed(x, gain), jnp.arange(ROWS)
    q = turned(matmul(a, wq).reshape(ROWS, HEADS, HEAD), place, THETA).reshape(ROWS, KV_HEADS, -1, HEAD)
    k = turned(matmul(a, wk).reshape(ROWS, KV_HEADS, HEAD), place, THETA)
    v = matmul(a, wv).reshape(ROWS, KV_HEADS, HEAD)
    seen = attention(q, k, v).reshape(ROWS, HEADS * HEAD)
    return (x.astype(jnp.float32) + jnp.dot(seen, wo, preferred_element_type=jnp.float32)).astype(jnp.bfloat16)
```

```python
import functools

import jax
import jax.numpy as jnp
import numpy as np
from jax import lax
from jax.experimental import pallas as pl
from jax.experimental.pallas import tpu as pltpu
from jax.sharding import PartitionSpec as P

MESH = pl.DeviceIdType.MESH
NEG = -1e30
HIDDEN = 2 * NEG
HEAD = 128
THETA = 10000
T = 512
D = 5120
W = 512
E = HEAD**-0.5 * 1.4426950408889634
VR = 136
BF, F32 = jnp.bfloat16, jnp.float32


def dot(a, b, ca, cb):
    return lax.dot_general(a, b, (((ca,), (cb,)), ((), ())), preferred_element_type=F32)


def tables():
    half = HEAD // 2
    freq = np.float64(THETA) ** (-np.arange(half) / half)
    near = np.arange(T)[:, None] * np.concatenate([freq, freq])
    far = (np.arange(8) * T)[:, None] * np.concatenate([freq, freq])
    return [np.concatenate([np.cos(a), np.sin(a)], 0).astype(np.float32) for a in (near, far)]


def fused(x_hbm, gain_ref, near_hbm, far_ref, wq_hbm, wk_hbm, wv_hbm, seen_hbm,
          x_s, a_s, w_s, z_s, near_s, cos_s, sin_s, q_s, k_s, v_s, vt_s, o_s, top_s, acc_s,
          x_sem, near_sem, w_sem, o_sem, kv_send, kv_recv, far_send, far_recv, q_send, q_recv, out_send, out_recv):
    me = lax.axis_index("sp")
    c, chip = lax.rem(me, 2), lax.div(me, 2)
    partner = me + 1 - 2 * c
    straight = lax.rem(me + 2, 4)
    diagonal = lax.rem(partner + 2, 4)

    def wblock(j):
        if j < 4:
            half = 1 - c if j < 2 else c
            src = (wk_hbm if j % 2 == 0 else wv_hbm).at[:, pl.ds(pl.multiple_of(half * W, W), W)]
            return pltpu.make_async_copy(src, w_s.at[j % 2], w_sem.at[j % 2])
        raise ValueError

    def qblock(n):
        half = jnp.where(n < 4, 1 - c, c)
        at = pl.multiple_of(half * 2048 + lax.rem(n, 4) * W, W)
        return pltpu.make_async_copy(wq_hbm.at[:, pl.ds(at, W)], w_s.at[lax.rem(n, 2)], w_sem.at[lax.rem(n, 2)])

    def rcopy(src, dst, send, recv, device):
        return pltpu.make_async_remote_copy(src_ref=src, dst_ref=dst, send_sem=send, recv_sem=recv,
                                            device_id={"sp": device}, device_id_type=MESH)

    rows = T // 4
    xcopies = [pltpu.make_async_copy(x_hbm.at[pl.ds(r * rows, rows)], x_s.at[pl.ds(r * rows, rows)], x_sem.at[r]) for r in range(4)]
    for cp in xcopies:
        cp.start()
    wblock(0).start()
    near_copy = pltpu.make_async_copy(near_hbm, near_s, near_sem)
    near_copy.start()
    wblock(1).start()

    barrier = pltpu.get_barrier_semaphore()
    for d in (partner, straight, diagonal):
        pl.semaphore_signal(barrier, inc=1, device_id={"sp": d}, device_id_type=MESH)

    def norm(r, _):
        here = pl.ds(pl.multiple_of(r * 16, 16), 16)
        wide = x_s[here, :].astype(F32)
        scale = lax.rsqrt(jnp.mean(wide * wide, -1, keepdims=True) + 1e-6)
        a_s[here, :] = (wide * scale * gain_ref[...].astype(F32)).astype(BF)

    for r in range(4):
        xcopies[r].wait()
        lax.fori_loop(r * rows // 16, (r + 1) * rows // 16, norm, None)

    near_copy.wait()
    c0, s0 = far_ref[pl.ds(me, 1), :], far_ref[pl.ds(me + 8, 1), :]
    sign = jnp.where(lax.broadcasted_iota(jnp.int32, (1, HEAD), 1) < HEAD // 2, -1.0, 1.0)
    cos_s[...] = near_s[:T] * c0 - near_s[T:] * s0
    sin_s[...] = (near_s[T:] * c0 + near_s[:T] * s0) * sign

    def project(slot, out):
        z_s[out] = dot(a_s[...], w_s[slot], 1, 0).astype(BF)

    def turn(zslot, ref, lead):
        for h in range(4):
            z = z_s[zslot, :, h * HEAD:(h + 1) * HEAD].astype(F32)
            ref[(*lead, h)] = (z * cos_s[...] + pltpu.roll(z, HEAD // 2, 1) * sin_s[...]).astype(BF)

    def values(zslot, ref, lead):
        for h in range(4):
            ref[(*lead, h, slice(0, HEAD))] = z_s[zslot, :, h * HEAD:(h + 1) * HEAD].T

    for s in range(4):
        for h in range(4):
            v_s[s, h, HEAD:, :] = jnp.ones((16, T), BF)

    near_k = rcopy(k_s.at[4], k_s.at[c], kv_send.at[0], kv_recv.at[0], partner)
    near_v = rcopy(vt_s, v_s.at[c, :, pl.ds(0, HEAD)], kv_send.at[1], kv_recv.at[1], partner)
    far = [
        rcopy(k_s.at[4], k_s.at[2 + c], far_send.at[0], far_recv.at[c, 0], diagonal),
        rcopy(vt_s, v_s.at[2 + c, :, pl.ds(0, HEAD)], far_send.at[1], far_recv.at[c, 1], diagonal),
        rcopy(k_s.at[c], k_s.at[2 + c], far_send.at[2], far_recv.at[c, 0], straight),
        rcopy(v_s.at[c, :, pl.ds(0, HEAD)], v_s.at[2 + c, :, pl.ds(0, HEAD)], far_send.at[3], far_recv.at[c, 1], straight),
    ]

    def send_far(n):
        @pl.when(chip == 0)
        def _():
            far[n].start()

    wblock(0).wait()
    project(0, 0)
    wblock(2).start()
    wblock(1).wait()
    pl.semaphore_wait(barrier, 3)
    project(1, 1)
    turn(0, k_s, (4,))
    wblock(3).start()
    near_k.start()
    send_far(0)
    wblock(2).wait()
    project(0, 0)
    values(1, vt_s, ())
    qblock(0).start()
    near_v.start()
    send_far(1)
    wblock(3).wait()
    project(1, 1)
    turn(0, k_s, (c,))
    qblock(1).start()
    send_far(2)
    qblock(0).wait()
    project(0, 0)
    values(1, v_s, (c,))
    qblock(2).start()
    send_far(3)

    def qcopy(i):
        return rcopy(q_s.at[2, i], q_s.at[c, i], q_send.at[i], q_recv.at[i], partner)

    def queries(n, _):
        qblock(n).wait()
        project(lax.rem(n, 2), lax.rem(n, 2))
        turn(lax.rem(n + 1, 2), q_s, (jnp.where(n <= 4, 2, c), lax.rem(n - 1, 4)))

        @pl.when(n < 6)
        def _():
            qblock(n + 2).start()

        @pl.when(n <= 4)
        def _():
            qcopy(n - 1).start()

    lax.fori_loop(1, 8, queries, None)
    turn(1, q_s, (c, 3))

    later = lax.broadcasted_iota(jnp.int32, (256, 256), 1) >= lax.broadcasted_iota(jnp.int32, (256, 256), 0)

    def attend(items, i, done=None):
        n = len(items)
        scores, weights, keeps = {}, {}, {}
        cols = {"full": slice(0, T), "left": slice(0, 256), "right": slice(256, T)}
        keys = {"full": T, "left": 256, "right": T}

        def qk(m):
            t, h, s, _, kind = items[m]
            scores[m] = dot(k_s[s, i, 0:keys[kind]], q_s[t, i, h, cols[kind]], 1, 1)

        def soft(m):
            t, h, s, first, kind = items[m]
            x, row = scores.pop(m), t * 16 + i * 4 + h
            if kind == "left":
                x = jnp.where(later, x, HIDDEN)
            if kind == "right":
                x = jnp.concatenate([x[:256], jnp.where(later, x[256:], HIDDEN)], 0)
            top = x.max(axis=0, keepdims=True)
            if not first:
                old = top_s[pl.ds(row, 1), cols[kind]]
                top = jnp.maximum(old, top)
                keeps[m] = jnp.exp2((old - top) * E)
            top_s[pl.ds(row, 1), cols[kind]] = top
            weights[m] = jnp.exp2((x - top) * E).astype(BF)

        def pv(m):
            t, h, s, first, kind = items[m]
            row = t * 16 + i * 4 + h
            new = dot(v_s[s, i, :, 0:keys[kind]], weights.pop(m), 1, 0)[:VR]
            if not first:
                new = acc_s[row, :, cols[kind]] * keeps.pop(m) + new
            if done is None:
                acc_s[row, :, cols[kind]] = new
            else:
                done(t, h, new)

        qk(0)
        qk(1)
        for m in range(n):
            soft(m)
            if m + 2 < n:
                qk(m + 2)
            if m >= 1:
                pv(m - 1)
        pv(n - 1)


    near_k.wait_recv()
    near_v.wait_recv()
    for i in range(4):
        qcopy(i).wait_recv()

    def local(i, _):
        attend([(0, h, 0, True, side) for h in range(4) for side in ("left", "right")]
               + [(1, h, 0, True, "full") for h in range(4)]
               + [(1, h, 1, False, side) for h in range(4) for side in ("left", "right")], i)

    lax.fori_loop(0, 4, local, None)

    def out_copies(i):
        par = lax.rem(i, 2)
        at = pl.multiple_of(c * 2048 + i * W, W)
        return [(rcopy(o_s2(par, 1 - c, h), seen_hbm.at[:, pl.ds(pl.multiple_of(at + h * HEAD, HEAD), HEAD)],
                       out_send.at[par, h], out_recv.at[i, h], partner),
                 pltpu.make_async_copy(o_s2(par, c, h), seen_hbm.at[:, pl.ds(pl.multiple_of(at + h * HEAD, HEAD), HEAD)],
                                       o_sem.at[par, h])) for h in range(4)]

    def o_s2(par, t, h):
        return o_s.at[par * 2 + t, h]

    def emit(i, work):
        par = lax.rem(i, 2)

        @pl.when(i >= 2)
        def _():
            for away, home in out_copies(i - 2):
                away.wait_send()
                home.wait()

        work(i, lambda t, h, total: o_s.__setitem__((par * 2 + t, h), (total[:HEAD] * (1 / total[HEAD:HEAD + 1])).T.astype(BF)))
        for away, home in out_copies(i):
            away.start()
            home.start()

    @pl.when(chip == 1)
    def _():
        def wait_far(s):
            rcopy(k_s.at[4], k_s.at[2 + s], far_send.at[0], far_recv.at[s, 0], straight).wait_recv()
            rcopy(vt_s, v_s.at[2 + s, :, pl.ds(0, HEAD)], far_send.at[1], far_recv.at[s, 1], straight).wait_recv()

        wait_far(1 - c)

        def other(i, _):
            attend([(t, h, 3 - c, False, "full") for t in range(2) for h in range(4)], i)

        lax.fori_loop(0, 4, other, None)
        wait_far(c)

        def last(i, _):
            emit(i, lambda i, put: attend([(t, h, 2 + c, False, "full") for t in range(2) for h in range(4)], i, put))

        lax.fori_loop(0, 4, last, None)

    @pl.when(chip == 0)
    def _():
        def last(i, _):
            def work(i, put):
                for t in range(2):
                    for h in range(4):
                        put(t, h, acc_s[t * 16 + i * 4 + h])

            emit(i, work)

        lax.fori_loop(0, 4, last, None)
        for n in range(4):
            far[n].wait_send()

    near_k.wait_send()
    near_v.wait_send()
    for i in range(4):
        qcopy(i).wait_send()
    for i in (2, 3):
        for away, home in out_copies(i):
            away.wait_send()
            home.wait()
    for i in range(4):
        for away, _ in out_copies(i):
            away.wait_recv()


def attention(x, gain, wq, wk, wv):
    near, far = tables()
    hbm, vmem = pl.BlockSpec(memory_space=pl.ANY), pl.BlockSpec(memory_space=pltpu.VMEM)
    dma = pltpu.SemaphoreType.DMA
    return pl.pallas_call(
        fused,
        out_shape=jax.ShapeDtypeStruct((T, 4096), BF),
        in_specs=[hbm, vmem, hbm, vmem, hbm, hbm, hbm],
        out_specs=hbm,
        scratch_shapes=[
            pltpu.VMEM((T, D), BF), pltpu.VMEM((T, D), BF), pltpu.VMEM((2, D, W), BF), pltpu.VMEM((2, T, W), BF),
            pltpu.VMEM((2 * T, HEAD), F32), pltpu.VMEM((T, HEAD), F32), pltpu.VMEM((T, HEAD), F32),
            pltpu.VMEM((3, 4, 4, T, HEAD), BF), pltpu.VMEM((5, 4, T, HEAD), BF), pltpu.VMEM((4, 4, HEAD + 16, T), BF),
            pltpu.VMEM((4, HEAD, T), BF), pltpu.VMEM((4, 4, T, HEAD), BF),
            pltpu.VMEM((32, T), F32), pltpu.VMEM((32, VR, T), F32),
            dma((4,)), dma, dma((2,)), dma((2, 4)),
            dma((2,)), dma((2,)), dma((4,)), dma((2, 2)), dma((4,)), dma((4,)), dma((2, 4)), dma((4, 4)),
        ],
        compiler_params=pltpu.CompilerParams(collective_id=0, has_side_effects=True, vmem_limit_bytes=63 * 2**20),
        cost_estimate=pl.CostEstimate(flops=45 * 10**9, bytes_accessed=80 * 10**6, transcendentals=30 * 10**6),
        name="project_attend",
    )(x, gain.reshape(1, D), jnp.asarray(near), jnp.asarray(far), wq, wk, wv)


def out_kernel(s_ref, w_ref, x_ref, y_ref):
    y = dot(s_ref[...], w_ref[...], 1, 0)
    y_ref[...] = (x_ref[...].astype(F32) + y).astype(BF)


def out_project(seen, wo, x):
    k = seen.shape[1]
    return pl.pallas_call(
        out_kernel,
        out_shape=jax.ShapeDtypeStruct((T, D), BF),
        grid=(D // W,),
        in_specs=[pl.BlockSpec((T, k), lambda j: (0, 0)), pl.BlockSpec((k, W), lambda j: (0, j)), pl.BlockSpec((T, W), lambda j: (0, j))],
        out_specs=pl.BlockSpec((T, W), lambda j: (0, j)),
        compiler_params=pltpu.CompilerParams(dimension_semantics=("arbitrary",), vmem_limit_bytes=56 * 2**20),
        cost_estimate=pl.CostEstimate(flops=2 * T * k * D, bytes_accessed=2 * (k * D + T * k + 2 * T * D), transcendentals=0),
        name="out_project",
    )(seen, wo, x)


def solution(mesh):
    def step(x, gain, wq, wk, wv, wo):
        return out_project(attention(x, gain, wq, wk, wv), wo, x)

    tokens, whole = P(("dp", "sp"), None), P(None, None)
    return jax.shard_map(step, mesh=mesh, in_specs=(tokens, P(None), whole, whole, whole, whole), out_specs=tokens, check_vma=False)
```

```python
import functools

import jax
import jax.numpy as jnp
import numpy as np
from jax import lax
from jax.experimental import pallas as pl
from jax.experimental.pallas import tpu as pltpu
from jax.sharding import PartitionSpec as P

MESH = pl.DeviceIdType.MESH
NEG = -1e30
HIDDEN = 2 * NEG
HEAD = 128
THETA = 10000
T = 512
D = 5120
W = 512
E = HEAD**-0.5 * 1.4426950408889634
VR = 136
BF, F32 = jnp.bfloat16, jnp.float32


def dot(a, b, ca, cb):
    return lax.dot_general(a, b, (((ca,), (cb,)), ((), ())), preferred_element_type=F32)


def tables():
    half = HEAD // 2
    freq = np.float64(THETA) ** (-np.arange(half) / half)
    near = np.arange(T)[:, None] * np.concatenate([freq, freq])
    far = (np.arange(8) * T)[:, None] * np.concatenate([freq, freq])
    return [np.concatenate([np.cos(a), np.sin(a)], 0).astype(np.float32) for a in (near, far)]


def fused(x_hbm, gain_ref, near_hbm, far_ref, wq_hbm, wk_hbm, wv_hbm, seen_hbm,
          x_s, a_s, w_s, z_s, near_s, cos_s, sin_s, q_s, k_s, v_s, vt_s, o_s, top_s, acc_s,
          x_sem, near_sem, w_sem, o_sem, kv_send, kv_recv, far_send, far_recv, q_send, q_recv, out_send, out_recv):
    me = lax.axis_index("sp")
    c, chip = lax.rem(me, 2), lax.div(me, 2)
    partner = me + 1 - 2 * c
    straight = lax.rem(me + 2, 4)
    diagonal = lax.rem(partner + 2, 4)

    def wblock(j):
        if j < 4:
            half = 1 - c if j < 2 else c
            src = (wk_hbm if j % 2 == 0 else wv_hbm).at[:, pl.ds(pl.multiple_of(half * W, W), W)]
            return pltpu.make_async_copy(src, w_s.at[j % 2], w_sem.at[j % 2])
        raise ValueError

    def qblock(n):
        half = jnp.where(n < 4, 1 - c, c)
        at = pl.multiple_of(half * 2048 + lax.rem(n, 4) * W, W)
        return pltpu.make_async_copy(wq_hbm.at[:, pl.ds(at, W)], w_s.at[lax.rem(n, 2)], w_sem.at[lax.rem(n, 2)])

    def rcopy(src, dst, send, recv, device):
        return pltpu.make_async_remote_copy(src_ref=src, dst_ref=dst, send_sem=send, recv_sem=recv,
                                            device_id={"sp": device}, device_id_type=MESH)

    rows = T // 4
    xcopies = [pltpu.make_async_copy(x_hbm.at[pl.ds(r * rows, rows)], x_s.at[pl.ds(r * rows, rows)], x_sem.at[r]) for r in range(4)]
    for cp in xcopies:
        cp.start()
    near_copy = pltpu.make_async_copy(near_hbm, near_s, near_sem)
    near_copy.start()
    deep = D // 2
    first = [pltpu.make_async_copy(wk_hbm.at[pl.ds(n * deep, deep), pl.ds(pl.multiple_of((1 - c) * W, W), W)],
                                   w_s.at[0, pl.ds(n * deep, deep)], w_sem.at[2 * n]) for n in range(2)]

    barrier = pltpu.get_barrier_semaphore()
    for d in (partner, straight, diagonal):
        pl.semaphore_signal(barrier, inc=1, device_id={"sp": d}, device_id_type=MESH)

    def norm(r, _):
        here = pl.ds(pl.multiple_of(r * 64, 64), 64)
        cols = [slice(n * HEAD, (n + 1) * HEAD) for n in range(D // HEAD)]
        total = jnp.zeros((64, HEAD), F32)
        for n in cols:
            wide = x_s[here, n].astype(F32)
            total += wide * wide
        scale = jnp.broadcast_to(lax.rsqrt(jnp.sum(total, -1, keepdims=True) * (1 / D) + 1e-6), (64, HEAD))
        for n in cols:
            a_s[here, n] = (x_s[here, n].astype(F32) * scale * gain_ref[n].astype(F32).reshape(1, HEAD)).astype(BF)

    for r in range(4):
        xcopies[r].wait()
        if r == 1:
            first[0].start()
        if r == 3:
            first[1].start()
            wblock(1).start()
        lax.fori_loop(r * rows // 64, (r + 1) * rows // 64, norm, None)

    near_copy.wait()
    c0, s0 = far_ref[pl.ds(me, 1), :], far_ref[pl.ds(me + 8, 1), :]
    sign = jnp.where(lax.broadcasted_iota(jnp.int32, (1, HEAD), 1) < HEAD // 2, -1.0, 1.0)
    cos_s[...] = near_s[:T] * c0 - near_s[T:] * s0
    sin_s[...] = (near_s[T:] * c0 + near_s[:T] * s0) * sign

    def project(slot, out):
        z_s[out] = dot(a_s[...], w_s[slot], 1, 0).astype(BF)

    def turn(zslot, ref, lead):
        for h in range(4):
            z = z_s[zslot, :, h * HEAD:(h + 1) * HEAD].astype(F32)
            ref[(*lead, h)] = (z * cos_s[...] + pltpu.roll(z, HEAD // 2, 1) * sin_s[...]).astype(BF)

    def values(zslot, ref, lead):
        for h in range(4):
            ref[(*lead, h, slice(0, HEAD))] = z_s[zslot, :, h * HEAD:(h + 1) * HEAD].T

    for s in range(4):
        for h in range(4):
            v_s[s, h, HEAD:, :] = jnp.ones((16, T), BF)

    near_k = rcopy(k_s.at[4], k_s.at[c], kv_send.at[0], kv_recv.at[0], partner)
    near_v = rcopy(vt_s, v_s.at[c, :, pl.ds(0, HEAD)], kv_send.at[1], kv_recv.at[1], partner)
    far = [
        rcopy(k_s.at[4], k_s.at[2 + c], far_send.at[0], far_recv.at[c, 0], diagonal),
        rcopy(vt_s, v_s.at[2 + c, :, pl.ds(0, HEAD)], far_send.at[1], far_recv.at[c, 1], diagonal),
        rcopy(k_s.at[c], k_s.at[2 + c], far_send.at[2], far_recv.at[c, 0], straight),
        rcopy(v_s.at[c, :, pl.ds(0, HEAD)], v_s.at[2 + c, :, pl.ds(0, HEAD)], far_send.at[3], far_recv.at[c, 1], straight),
    ]

    def send_far(n):
        @pl.when(chip == 0)
        def _():
            far[n].start()

    first[0].wait()
    acc_s[0:4, 0:128, :] = dot(a_s[:, :deep], w_s[0, :deep], 1, 0).reshape(4, 128, W)
    first[1].wait()
    z_s[0] = (acc_s[0:4, 0:128, :].reshape(T, W) + dot(a_s[:, deep:], w_s[0, deep:], 1, 0)).astype(BF)
    wblock(2).start()
    wblock(1).wait()
    pl.semaphore_wait(barrier, 3)
    project(1, 1)
    turn(0, k_s, (4,))
    wblock(3).start()
    near_k.start()
    send_far(0)
    wblock(2).wait()
    project(0, 0)
    values(1, vt_s, ())
    qblock(0).start()
    near_v.start()
    send_far(1)
    wblock(3).wait()
    project(1, 1)
    turn(0, k_s, (c,))
    qblock(1).start()
    send_far(2)
    qblock(0).wait()
    project(0, 0)
    values(1, v_s, (c,))
    qblock(2).start()
    send_far(3)

    def qcopy(i):
        return rcopy(q_s.at[2, i], q_s.at[c, i], q_send.at[i], q_recv.at[i], partner)

    def queries(n, _):
        qblock(n).wait()
        project(lax.rem(n, 2), lax.rem(n, 2))
        turn(lax.rem(n + 1, 2), q_s, (jnp.where(n <= 4, 2, c), lax.rem(n - 1, 4)))

        @pl.when(n < 6)
        def _():
            qblock(n + 2).start()

        @pl.when(n <= 4)
        def _():
            qcopy(n - 1).start()

    lax.fori_loop(1, 8, queries, None)
    turn(1, q_s, (c, 3))

    later = lax.broadcasted_iota(jnp.int32, (256, T), 1) % 256 >= lax.broadcasted_iota(jnp.int32, (256, T), 0)

    def attend(items, i, done=None):
        n = len(items)
        scores, weights, keeps = {}, {}, {}
        cols = {"full": slice(0, T), "left": slice(0, 256), "right": slice(256, T)}
        keys = {"full": T, "left": 256, "right": T}

        def joined(parts, axis):
            return parts[0] if len(parts) == 1 else jnp.concatenate(parts, axis)

        def split(x, hs):
            wide = x.shape[-1] // len(hs)
            return [x[..., n * wide:(n + 1) * wide] for n in range(len(hs))]

        def qk(m):
            t, hs, s, _, kind = items[m]
            scores[m] = dot(k_s[s, i, 0:keys[kind]], joined([q_s[t, i, h, cols[kind]] for h in hs], 0), 1, 1)

        def soft(m):
            t, hs, s, first, kind = items[m]
            x = scores.pop(m)
            if kind == "left":
                x = jnp.where(later, x, HIDDEN)
            if kind == "right":
                x = jnp.concatenate([x[:256], jnp.where(later, x[256:], HIDDEN)], 0)
            top = x.max(axis=0, keepdims=True)
            rows = [t * 16 + i * 4 + h for h in hs]
            if not first:
                old = joined([top_s[pl.ds(row, 1), cols[kind]] for row in rows], 1)
                top = jnp.maximum(old, top)
                keeps[m] = jnp.exp2((old - top) * E)
            for row, part in zip(rows, split(top, hs)):
                top_s[pl.ds(row, 1), cols[kind]] = part
            weights[m] = jnp.exp2((x - top) * E).astype(BF)

        def pv(m):
            t, hs, s, first, kind = items[m]
            new = split(dot(v_s[s, i, :, 0:keys[kind]], weights.pop(m), 1, 0)[:VR], hs)
            keep = [None] * len(hs) if first else split(keeps.pop(m), hs)
            for h, part, kept in zip(hs, new, keep):
                row = t * 16 + i * 4 + h
                if not first:
                    part = acc_s[row, :, cols[kind]] * kept + part
                if done is None:
                    acc_s[row, :, cols[kind]] = part
                else:
                    done(t, h, part)

        qk(0)
        qk(1)
        for m in range(n):
            soft(m)
            if m + 2 < n:
                qk(m + 2)
            if m >= 1:
                pv(m - 1)
        pv(n - 1)

    near_k.wait_recv()
    near_v.wait_recv()
    for i in range(4):
        qcopy(i).wait_recv()

    def local(i, _):
        pairs = ((0, 1), (2, 3))
        attend([(0, hs, 0, True, side) for hs in pairs for side in ("left", "right")]
               + [(1, (h,), 0, True, "full") for h in range(4)]
               + [(1, hs, 1, False, side) for hs in pairs for side in ("left", "right")], i)

    lax.fori_loop(0, 4, local, None)

    def out_copies(i):
        par = lax.rem(i, 2)
        at = pl.multiple_of(c * 2048 + i * W, W)
        return [(rcopy(o_s2(par, 1 - c, h), seen_hbm.at[:, pl.ds(pl.multiple_of(at + h * HEAD, HEAD), HEAD)],
                       out_send.at[par, h], out_recv.at[i, h], partner),
                 pltpu.make_async_copy(o_s2(par, c, h), seen_hbm.at[:, pl.ds(pl.multiple_of(at + h * HEAD, HEAD), HEAD)],
                                       o_sem.at[par, h])) for h in range(4)]

    def o_s2(par, t, h):
        return o_s.at[par * 2 + t, h]

    def emit(i, work):
        par = lax.rem(i, 2)

        @pl.when(i >= 2)
        def _():
            for away, home in out_copies(i - 2):
                away.wait_send()
                home.wait()

        work(i, lambda t, h, total: o_s.__setitem__((par * 2 + t, h), (total[:HEAD] * (1 / total[HEAD:HEAD + 1])).T.astype(BF)))
        for away, home in out_copies(i):
            away.start()
            home.start()

    @pl.when(chip == 1)
    def _():
        def wait_far(s):
            rcopy(k_s.at[4], k_s.at[2 + s], far_send.at[0], far_recv.at[s, 0], straight).wait_recv()
            rcopy(vt_s, v_s.at[2 + s, :, pl.ds(0, HEAD)], far_send.at[1], far_recv.at[s, 1], straight).wait_recv()

        wait_far(1 - c)

        def other(i, _):
            attend([(t, (h,), 3 - c, False, "full") for t in range(2) for h in range(4)], i)

        lax.fori_loop(0, 4, other, None)
        wait_far(c)

        def last(i, _):
            emit(i, lambda i, put: attend([(t, (h,), 2 + c, False, "full") for t in range(2) for h in range(4)], i, put))

        lax.fori_loop(0, 4, last, None)

    @pl.when(chip == 0)
    def _():
        def last(i, _):
            def work(i, put):
                for t in range(2):
                    for h in range(4):
                        put(t, h, acc_s[t * 16 + i * 4 + h])

            emit(i, work)

        lax.fori_loop(0, 4, last, None)
        for n in range(4):
            far[n].wait_send()

    near_k.wait_send()
    near_v.wait_send()
    for i in range(4):
        qcopy(i).wait_send()
    for i in (2, 3):
        for away, home in out_copies(i):
            away.wait_send()
            home.wait()
    for i in range(4):
        for away, _ in out_copies(i):
            away.wait_recv()


def attention(x, gain, wq, wk, wv):
    near, far = tables()
    hbm, vmem = pl.BlockSpec(memory_space=pl.ANY), pl.BlockSpec(memory_space=pltpu.VMEM)
    dma = pltpu.SemaphoreType.DMA
    return pl.pallas_call(
        fused,
        out_shape=jax.ShapeDtypeStruct((T, 4096), BF),
        in_specs=[hbm, vmem, hbm, vmem, hbm, hbm, hbm],
        out_specs=hbm,
        scratch_shapes=[
            pltpu.VMEM((T, D), BF), pltpu.VMEM((T, D), BF), pltpu.VMEM((2, D, W), BF), pltpu.VMEM((2, T, W), BF),
            pltpu.VMEM((2 * T, HEAD), F32), pltpu.VMEM((T, HEAD), F32), pltpu.VMEM((T, HEAD), F32),
            pltpu.VMEM((3, 4, 4, T, HEAD), BF), pltpu.VMEM((5, 4, T, HEAD), BF), pltpu.VMEM((4, 4, HEAD + 16, T), BF),
            pltpu.VMEM((4, HEAD, T), BF), pltpu.VMEM((4, 4, T, HEAD), BF),
            pltpu.VMEM((32, T), F32), pltpu.VMEM((32, VR, T), F32),
            dma((4,)), dma, dma((3,)), dma((2, 4)),
            dma((2,)), dma((2,)), dma((4,)), dma((2, 2)), dma((4,)), dma((4,)), dma((2, 4)), dma((4, 4)),
        ],
        compiler_params=pltpu.CompilerParams(collective_id=0, has_side_effects=True, vmem_limit_bytes=63 * 2**20),
        cost_estimate=pl.CostEstimate(flops=45 * 10**9, bytes_accessed=80 * 10**6, transcendentals=30 * 10**6),
        name="project_attend",
    )(x, gain, jnp.asarray(near), jnp.asarray(far), wq, wk, wv)


def out_kernel(seen_hbm, w_hbm, x_hbm, y_hbm, s_s, w_s, x_s, z_s, y_s, first_sem, w_sem, x_sem, y_sem):
    k, blocks, slots = s_s.shape[1], D // W, 3
    deep = k // 4
    pieces = []
    for n in range(4):
        here = pl.ds(n * deep, deep)
        pieces += [pltpu.make_async_copy(seen_hbm.at[:, here], s_s.at[:, here], first_sem.at[0, n]),
                   pltpu.make_async_copy(w_hbm.at[here, pl.ds(0, W)], w_s.at[0, here], first_sem.at[1, n])]

    def weights(j):
        at = pl.multiple_of(j * W, W)
        return pltpu.make_async_copy(w_hbm.at[:, pl.ds(at, W)], w_s.at[lax.rem(j, slots)], w_sem.at[lax.rem(j, slots)])

    def result(j):
        at = pl.multiple_of(j * W, W)
        return pltpu.make_async_copy(y_s.at[lax.rem(j, 2)], y_hbm.at[:, pl.ds(at, W)], y_sem.at[lax.rem(j, 2)])

    def finish(j):
        here = pl.ds(pl.multiple_of(j * W, W), W)
        y_s[lax.rem(j, 2)] = (x_s[:, here].astype(F32) + z_s[lax.rem(j, 2)]).astype(BF)

    xcopy = pltpu.make_async_copy(x_hbm, x_s, x_sem)
    for cp in pieces:
        cp.start()
    weights(1).start()
    xcopy.start()
    weights(2).start()
    for n in range(4):
        pieces[2 * n].wait()
        pieces[2 * n + 1].wait()
        here = slice(n * deep, (n + 1) * deep)
        part = dot(s_s[:, here], w_s[0, here], 1, 0)
        z_s[0] = part if n == 0 else z_s[0] + part
    xcopy.wait()

    def block(j, _):
        weights(j).wait()
        z_s[lax.rem(j, 2)] = dot(s_s[...], w_s[lax.rem(j, slots)], 1, 0)
        finish(j - 1)

        @pl.when(j + 2 < blocks)
        def _():
            weights(j + 2).start()

        result(j - 1).start()

        @pl.when(j >= 2)
        def _():
            result(j - 2).wait()

    lax.fori_loop(1, blocks, block, None)
    finish(blocks - 1)
    result(blocks - 1).start()
    result(blocks - 2).wait()
    result(blocks - 1).wait()


def out_project(seen, wo, x):
    k = seen.shape[1]
    hbm, dma = pl.BlockSpec(memory_space=pl.ANY), pltpu.SemaphoreType.DMA
    return pl.pallas_call(
        out_kernel,
        out_shape=jax.ShapeDtypeStruct((T, D), BF),
        in_specs=[hbm] * 3,
        out_specs=hbm,
        scratch_shapes=[pltpu.VMEM((T, k), BF), pltpu.VMEM((3, k, W), BF), pltpu.VMEM((T, D), BF), pltpu.VMEM((2, T, W), F32),
                        pltpu.VMEM((2, T, W), BF), dma((2, 4)), dma((3,)), dma, dma((2,))],
        compiler_params=pltpu.CompilerParams(vmem_limit_bytes=60 * 2**20),
        cost_estimate=pl.CostEstimate(flops=2 * T * k * D, bytes_accessed=2 * (k * D + T * k + 2 * T * D), transcendentals=0),
        name="out_project",
    )(seen, wo, x)


def solution(mesh):
    def step(x, gain, wq, wk, wv, wo):
        return out_project(attention(x, gain, wq, wk, wv), wo, x)

    tokens, whole = P(("dp", "sp"), None), P(None, None)
    return jax.shard_map(step, mesh=mesh, in_specs=(tokens, P(None), whole, whole, whole, whole), out_specs=tokens, check_vma=False)
```

```python
import functools

import jax
import jax.numpy as jnp
import numpy as np
from jax import lax
from jax.experimental import pallas as pl
from jax.experimental.pallas import tpu as pltpu
from jax.sharding import PartitionSpec as P

MESH = pl.DeviceIdType.MESH
NEG = -1e30
HIDDEN = 2 * NEG
HEAD = 128
THETA = 10000
T = 512
D = 5120
W = 512
E = HEAD**-0.5 * 1.4426950408889634
VR = 136
BF, F32 = jnp.bfloat16, jnp.float32


def dot(a, b, ca, cb):
    return lax.dot_general(a, b, (((ca,), (cb,)), ((), ())), preferred_element_type=F32)


def tables():
    half = HEAD // 2
    freq = np.float64(THETA) ** (-np.arange(half) / half)
    near = np.arange(T)[:, None] * np.concatenate([freq, freq])
    far = (np.arange(8) * T)[:, None] * np.concatenate([freq, freq])
    return [np.concatenate([np.cos(a), np.sin(a)], 0).astype(np.float32) for a in (near, far)]


def fused(x_hbm, gain_ref, near_hbm, far_ref, wq_hbm, wk_hbm, wv_hbm, seen_hbm,
          x_s, a_s, w_s, z_s, near_s, cos_s, sin_s, q_s, k_s, v_s, vt_s, o_s, top_s, acc_s,
          x_sem, near_sem, w_sem, o_sem, kv_send, kv_recv, far_send, far_recv, q_send, q_recv, out_send, out_recv):
    me = lax.axis_index("sp")
    c, chip = lax.rem(me, 2), lax.div(me, 2)
    partner = me + 1 - 2 * c
    straight = lax.rem(me + 2, 4)
    diagonal = lax.rem(partner + 2, 4)

    def wblock(j):
        if j < 4:
            half = 1 - c if j < 2 else c
            src = (wk_hbm if j % 2 == 0 else wv_hbm).at[:, pl.ds(pl.multiple_of(half * W, W), W)]
            return pltpu.make_async_copy(src, w_s.at[j % 2], w_sem.at[j % 2])
        raise ValueError

    def qblock(n):
        half = jnp.where(n < 4, 1 - c, c)
        at = pl.multiple_of(half * 2048 + lax.rem(n, 4) * W, W)
        return pltpu.make_async_copy(wq_hbm.at[:, pl.ds(at, W)], w_s.at[lax.rem(n, 2)], w_sem.at[lax.rem(n, 2)])

    def rcopy(src, dst, send, recv, device):
        return pltpu.make_async_remote_copy(src_ref=src, dst_ref=dst, send_sem=send, recv_sem=recv,
                                            device_id={"sp": device}, device_id_type=MESH)

    rows = T // 4
    xcopies = [pltpu.make_async_copy(x_hbm.at[pl.ds(r * rows, rows)], x_s.at[pl.ds(r * rows, rows)], x_sem.at[r]) for r in range(4)]
    for cp in xcopies:
        cp.start()
    near_copy = pltpu.make_async_copy(near_hbm, near_s, near_sem)
    near_copy.start()
    wblock(0).start()

    barrier = pltpu.get_barrier_semaphore()
    for d in (partner, straight, diagonal):
        pl.semaphore_signal(barrier, inc=1, device_id={"sp": d}, device_id_type=MESH)

    def norm(r, _):
        here = slice(r * 64, r * 64 + 64) if isinstance(r, int) else pl.ds(pl.multiple_of(r * 64, 64), 64)
        cols = [slice(n * HEAD, (n + 1) * HEAD) for n in range(D // HEAD)]
        total = jnp.zeros((64, HEAD), F32)
        for n in cols:
            wide = x_s[here, n].astype(F32)
            total += wide * wide
        scale = jnp.broadcast_to(lax.rsqrt(jnp.sum(total, -1, keepdims=True) * (1 / D) + 1e-6), (64, HEAD))
        for n in cols:
            a_s[here, n] = (x_s[here, n].astype(F32) * scale * gain_ref[n].astype(F32).reshape(1, HEAD)).astype(BF)

    for r in range(2):
        xcopies[r].wait()
        lax.fori_loop(r * rows // 64, (r + 1) * rows // 64, norm, None)
    xcopies[2].wait()
    xcopies[3].wait()
    wblock(1).start()

    near_copy.wait()
    c0, s0 = far_ref[pl.ds(me, 1), :], far_ref[pl.ds(me + 8, 1), :]
    sign = jnp.where(lax.broadcasted_iota(jnp.int32, (1, HEAD), 1) < HEAD // 2, -1.0, 1.0)
    cos_s[...] = near_s[:T] * c0 - near_s[T:] * s0
    sin_s[...] = (near_s[T:] * c0 + near_s[:T] * s0) * sign

    def project(slot, out):
        z_s[out] = dot(a_s[...], w_s[slot], 1, 0).astype(BF)

    def turn(zslot, ref, lead):
        for h in range(4):
            z = z_s[zslot, :, h * HEAD:(h + 1) * HEAD].astype(F32)
            ref[(*lead, h)] = (z * cos_s[...] + pltpu.roll(z, HEAD // 2, 1) * sin_s[...]).astype(BF)

    def values(zslot, ref, lead):
        for h in range(4):
            ref[(*lead, h, slice(0, HEAD))] = z_s[zslot, :, h * HEAD:(h + 1) * HEAD].T

    for s in range(4):
        for h in range(4):
            v_s[s, h, HEAD:, :] = jnp.ones((16, T), BF)

    near_k = rcopy(k_s.at[4], k_s.at[c], kv_send.at[0], kv_recv.at[0], partner)
    near_v = rcopy(vt_s, v_s.at[c, :, pl.ds(0, HEAD)], kv_send.at[1], kv_recv.at[1], partner)
    far = [
        rcopy(k_s.at[4], k_s.at[2 + c], far_send.at[0], far_recv.at[c, 0], diagonal),
        rcopy(vt_s, v_s.at[2 + c, :, pl.ds(0, HEAD)], far_send.at[1], far_recv.at[c, 1], diagonal),
        rcopy(k_s.at[c], k_s.at[2 + c], far_send.at[2], far_recv.at[c, 0], straight),
        rcopy(v_s.at[c, :, pl.ds(0, HEAD)], v_s.at[2 + c, :, pl.ds(0, HEAD)], far_send.at[3], far_recv.at[c, 1], straight),
    ]

    def send_far(n):
        @pl.when(chip == 0)
        def _():
            far[n].start()

    wblock(0).wait()
    z_s[0, :T // 2] = dot(a_s[:T // 2], w_s[0], 1, 0).astype(BF)
    for r in range(T // 128, T // 64):
        norm(r, None)
    z_s[0, T // 2:] = dot(a_s[T // 2:], w_s[0], 1, 0).astype(BF)
    wblock(2).start()
    wblock(1).wait()
    pl.semaphore_wait(barrier, 3)
    project(1, 1)
    turn(0, k_s, (4,))
    wblock(3).start()
    near_k.start()
    send_far(0)
    wblock(2).wait()
    project(0, 0)
    values(1, vt_s, ())
    qblock(0).start()
    near_v.start()
    send_far(1)
    wblock(3).wait()
    project(1, 1)
    turn(0, k_s, (c,))
    qblock(1).start()
    send_far(2)
    qblock(0).wait()
    project(0, 0)
    values(1, v_s, (c,))
    qblock(2).start()
    send_far(3)

    def qcopy(i):
        return rcopy(q_s.at[2, i], q_s.at[c, i], q_send.at[i], q_recv.at[i], partner)

    def queries(n, _):
        qblock(n).wait()
        turn(lax.rem(n + 1, 2), q_s, (jnp.where(n <= 4, 2, c), lax.rem(n - 1, 4)))
        project(lax.rem(n, 2), lax.rem(n, 2))

        @pl.when(n < 6)
        def _():
            qblock(n + 2).start()

        @pl.when(n <= 4)
        def _():
            qcopy(n - 1).start()

    lax.fori_loop(1, 8, queries, None)
    turn(1, q_s, (c, 3))

    later = lax.broadcasted_iota(jnp.int32, (256, T), 1) % 256 >= lax.broadcasted_iota(jnp.int32, (256, T), 0)

    def attend(items, i, done=None):
        n = len(items)
        scores, weights, keeps = {}, {}, {}
        cols = {"full": slice(0, T), "left": slice(0, 256), "right": slice(256, T)}
        keys = {"full": T, "left": 256, "right": T}

        def joined(parts, axis):
            return parts[0] if len(parts) == 1 else jnp.concatenate(parts, axis)

        def split(x, hs):
            wide = x.shape[-1] // len(hs)
            return [x[..., n * wide:(n + 1) * wide] for n in range(len(hs))]

        def qk(m):
            t, hs, s, _, kind = items[m]
            scores[m] = dot(k_s[s, i, 0:keys[kind]], joined([q_s[t, i, h, cols[kind]] for h in hs], 0), 1, 1)

        def soft(m):
            t, hs, s, first, kind = items[m]
            x = scores.pop(m)
            if kind == "left":
                x = jnp.where(later, x, HIDDEN)
            if kind == "right":
                x = jnp.concatenate([x[:256], jnp.where(later, x[256:], HIDDEN)], 0)
            top = x.max(axis=0, keepdims=True)
            rows = [t * 16 + i * 4 + h for h in hs]
            if not first:
                old = joined([top_s[pl.ds(row, 1), cols[kind]] for row in rows], 1)
                top = jnp.maximum(old, top)
                keeps[m] = jnp.exp2((old - top) * E)
            for row, part in zip(rows, split(top, hs)):
                top_s[pl.ds(row, 1), cols[kind]] = part
            weights[m] = jnp.exp2((x - top) * E).astype(BF)

        def pv(m):
            t, hs, s, first, kind = items[m]
            new = split(dot(v_s[s, i, :, 0:keys[kind]], weights.pop(m), 1, 0)[:VR], hs)
            keep = [None] * len(hs) if first else split(keeps.pop(m), hs)
            for h, part, kept in zip(hs, new, keep):
                row = t * 16 + i * 4 + h
                if not first:
                    part = acc_s[row, :, cols[kind]] * kept + part
                if done is None:
                    acc_s[row, :, cols[kind]] = part
                else:
                    done(t, h, part)

        qk(0)
        qk(1)
        for m in range(n):
            soft(m)
            if m + 2 < n:
                qk(m + 2)
            if m >= 1:
                pv(m - 1)
        pv(n - 1)

    near_k.wait_recv()
    near_v.wait_recv()
    for i in range(4):
        qcopy(i).wait_recv()

    def local(i, _):
        pairs = ((0, 1), (2, 3))
        attend([(0, hs, 0, True, side) for hs in pairs for side in ("left", "right")]
               + [(1, (h,), 0, True, "full") for h in range(4)]
               + [(1, hs, 1, False, side) for hs in pairs for side in ("left", "right")], i)

    lax.fori_loop(0, 4, local, None)

    def out_copies(i):
        par = lax.rem(i, 2)
        at = pl.multiple_of(c * 2048 + i * W, W)
        return [(rcopy(o_s2(par, 1 - c, h), seen_hbm.at[:, pl.ds(pl.multiple_of(at + h * HEAD, HEAD), HEAD)],
                       out_send.at[par, h], out_recv.at[i, h], partner),
                 pltpu.make_async_copy(o_s2(par, c, h), seen_hbm.at[:, pl.ds(pl.multiple_of(at + h * HEAD, HEAD), HEAD)],
                                       o_sem.at[par, h])) for h in range(4)]

    def o_s2(par, t, h):
        return o_s.at[par * 2 + t, h]

    def emit(i, work):
        par = lax.rem(i, 2)

        @pl.when(i >= 2)
        def _():
            for away, home in out_copies(i - 2):
                away.wait_send()
                home.wait()

        work(i, lambda t, h, total: o_s.__setitem__((par * 2 + t, h), (total[:HEAD] * (1 / total[HEAD:HEAD + 1])).T.astype(BF)))
        for away, home in out_copies(i):
            away.start()
            home.start()

    @pl.when(chip == 1)
    def _():
        def wait_far(s):
            rcopy(k_s.at[4], k_s.at[2 + s], far_send.at[0], far_recv.at[s, 0], straight).wait_recv()
            rcopy(vt_s, v_s.at[2 + s, :, pl.ds(0, HEAD)], far_send.at[1], far_recv.at[s, 1], straight).wait_recv()

        wait_far(1 - c)

        def other(i, _):
            attend([(t, (h,), 3 - c, False, "full") for t in range(2) for h in range(4)], i)

        lax.fori_loop(0, 4, other, None)
        wait_far(c)

        def last(i, _):
            emit(i, lambda i, put: attend([(t, (h,), 2 + c, False, "full") for t in range(2) for h in range(4)], i, put))

        lax.fori_loop(0, 4, last, None)

    @pl.when(chip == 0)
    def _():
        def last(i, _):
            def work(i, put):
                for t in range(2):
                    for h in range(4):
                        put(t, h, acc_s[t * 16 + i * 4 + h])

            emit(i, work)

        lax.fori_loop(0, 4, last, None)
        for n in range(4):
            far[n].wait_send()

    near_k.wait_send()
    near_v.wait_send()
    for i in range(4):
        qcopy(i).wait_send()
    for i in (2, 3):
        for away, home in out_copies(i):
            away.wait_send()
            home.wait()
    for i in range(4):
        for away, _ in out_copies(i):
            away.wait_recv()


def attention(x, gain, wq, wk, wv):
    near, far = tables()
    hbm, vmem = pl.BlockSpec(memory_space=pl.ANY), pl.BlockSpec(memory_space=pltpu.VMEM)
    dma = pltpu.SemaphoreType.DMA
    return pl.pallas_call(
        fused,
        out_shape=jax.ShapeDtypeStruct((T, 4096), BF),
        in_specs=[hbm, vmem, hbm, vmem, hbm, hbm, hbm],
        out_specs=hbm,
        scratch_shapes=[
            pltpu.VMEM((T, D), BF), pltpu.VMEM((T, D), BF), pltpu.VMEM((2, D, W), BF), pltpu.VMEM((2, T, W), BF),
            pltpu.VMEM((2 * T, HEAD), F32), pltpu.VMEM((T, HEAD), F32), pltpu.VMEM((T, HEAD), F32),
            pltpu.VMEM((3, 4, 4, T, HEAD), BF), pltpu.VMEM((5, 4, T, HEAD), BF), pltpu.VMEM((4, 4, HEAD + 16, T), BF),
            pltpu.VMEM((4, HEAD, T), BF), pltpu.VMEM((4, 4, T, HEAD), BF),
            pltpu.VMEM((32, T), F32), pltpu.VMEM((32, VR, T), F32),
            dma((4,)), dma, dma((2,)), dma((2, 4)),
            dma((2,)), dma((2,)), dma((4,)), dma((2, 2)), dma((4,)), dma((4,)), dma((2, 4)), dma((4, 4)),
        ],
        compiler_params=pltpu.CompilerParams(collective_id=0, has_side_effects=True, vmem_limit_bytes=63 * 2**20),
        cost_estimate=pl.CostEstimate(flops=45 * 10**9, bytes_accessed=80 * 10**6, transcendentals=30 * 10**6),
        name="project_attend",
    )(x, gain, jnp.asarray(near), jnp.asarray(far), wq, wk, wv)


def out_kernel(seen_hbm, w_hbm, x_hbm, y_hbm, s_s, w_s, x_s, z_s, y_s, first_sem, w_sem, x_sem, y_sem):
    k, blocks, slots = s_s.shape[1], D // W, 3
    parts = [(0, k // 8), (k // 8, k // 4), (3 * k // 8, 5 * k // 8)]
    pieces = []
    for n, (at, deep) in enumerate(parts):
        here = pl.ds(at, deep)
        pieces += [pltpu.make_async_copy(seen_hbm.at[:, here], s_s.at[:, here], first_sem.at[0, n]),
                   pltpu.make_async_copy(w_hbm.at[here, pl.ds(0, W)], w_s.at[0, here], first_sem.at[1, n])]

    def weights(j):
        at = pl.multiple_of(j * W, W)
        return pltpu.make_async_copy(w_hbm.at[:, pl.ds(at, W)], w_s.at[lax.rem(j, slots)], w_sem.at[lax.rem(j, slots)])

    def result(j):
        at = pl.multiple_of(j * W, W)
        return pltpu.make_async_copy(y_s.at[lax.rem(j, 2)], y_hbm.at[:, pl.ds(at, W)], y_sem.at[lax.rem(j, 2)])

    def finish(j):
        y_s[lax.rem(j, 2)] = (x_s[lax.rem(j, 3)].astype(F32) + z_s[lax.rem(j, 2)]).astype(BF)

    def residual(j):
        here = pl.ds(pl.multiple_of(j * W, W), W)
        return pltpu.make_async_copy(x_hbm.at[:, here], x_s.at[lax.rem(j, 3)], x_sem.at[lax.rem(j, 3)])

    for cp in pieces[:4]:
        cp.start()
    for n, (at, deep) in enumerate(parts):
        pieces[2 * n].wait()
        pieces[2 * n + 1].wait()
        if n == 0:
            pieces[4].start()
            pieces[5].start()
        if n == 1:
            weights(1).start()
            residual(0).start()
        here = slice(at, at + deep)
        part = dot(s_s[:, here], w_s[0, here], 1, 0)
        z_s[0] = part if n == 0 else z_s[0] + part
    residual(1).start()
    weights(2).start()

    def block(j, _):
        weights(j).wait()
        residual(j - 1).wait()
        finish(j - 1)
        z_s[lax.rem(j, 2)] = dot(s_s[...], w_s[lax.rem(j, slots)], 1, 0)

        @pl.when(j + 2 < blocks)
        def _():
            weights(j + 2).start()

        @pl.when(j + 1 < blocks)
        def _():
            residual(j + 1).start()

        result(j - 1).start()

        @pl.when(j >= 2)
        def _():
            result(j - 2).wait()

    lax.fori_loop(1, blocks, block, None)
    residual(blocks - 1).wait()
    finish(blocks - 1)
    result(blocks - 1).start()
    result(blocks - 2).wait()
    result(blocks - 1).wait()


def out_project(seen, wo, x):
    k = seen.shape[1]
    hbm, dma = pl.BlockSpec(memory_space=pl.ANY), pltpu.SemaphoreType.DMA
    return pl.pallas_call(
        out_kernel,
        out_shape=jax.ShapeDtypeStruct((T, D), BF),
        in_specs=[hbm] * 3,
        out_specs=hbm,
        scratch_shapes=[pltpu.VMEM((T, k), BF), pltpu.VMEM((3, k, W), BF), pltpu.VMEM((3, T, W), BF), pltpu.VMEM((2, T, W), F32),
                        pltpu.VMEM((2, T, W), BF), dma((2, 3)), dma((3,)), dma((3,)), dma((2,))],
        compiler_params=pltpu.CompilerParams(vmem_limit_bytes=60 * 2**20),
        cost_estimate=pl.CostEstimate(flops=2 * T * k * D, bytes_accessed=2 * (k * D + T * k + 2 * T * D), transcendentals=0),
        name="out_project",
    )(seen, wo, x)


def solution(mesh):
    def step(x, gain, wq, wk, wv, wo):
        return out_project(attention(x, gain, wq, wk, wv), wo, x)

    tokens, whole = P(("dp", "sp"), None), P(None, None)
    return jax.shard_map(step, mesh=mesh, in_specs=(tokens, P(None), whole, whole, whole, whole), out_specs=tokens, check_vma=False)
```

```python
import functools

import jax
import jax.numpy as jnp
import numpy as np
from jax import lax
from jax.experimental import pallas as pl
from jax.experimental.pallas import tpu as pltpu
from jax.sharding import PartitionSpec as P

MESH = pl.DeviceIdType.MESH
NEG = -1e30
HIDDEN = 2 * NEG
HEAD = 128
THETA = 10000
T = 512
D = 5120
W = 512
E = HEAD**-0.5 * 1.4426950408889634
VR = 136
BF, F32 = jnp.bfloat16, jnp.float32


def dot(a, b, ca, cb):
    return lax.dot_general(a, b, (((ca,), (cb,)), ((), ())), preferred_element_type=F32)


def tables():
    half = HEAD // 2
    freq = np.float64(THETA) ** (-np.arange(half) / half)
    near, far = np.arange(T)[:, None] * freq, (np.arange(8) * T)[:, None] * freq
    far = np.concatenate([far, far], 1)
    return [t.astype(np.float32) for t in (np.concatenate([np.cos(near), np.sin(near)], 1), np.concatenate([np.cos(far), np.sin(far)]))]


def fused(x_hbm, gain_ref, near_hbm, far_ref, wq_hbm, wk_hbm, wv_hbm, seen_hbm,
          x_s, a_s, w_s, z_s, near_s, cos_s, sin_s, q_s, k_s, v_s, vt_s, o_s, top_s, acc_s, qf_s, f_s,
          x_sem, near_sem, w_sem, o_sem, kv_send, kv_recv, far_send, far_recv, q_send, q_recv, out_send, out_recv,
          qf_send, qf_recv, f_send, f_recv):
    me = lax.axis_index("sp")
    c, chip = lax.rem(me, 2), lax.div(me, 2)
    partner = me + 1 - 2 * c
    straight = lax.rem(me + 2, 4)
    diagonal = lax.rem(partner + 2, 4)

    def wblock(j):
        if j < 4:
            half = 1 - c if j < 2 else c
            src = (wk_hbm if j % 2 == 0 else wv_hbm).at[:, pl.ds(pl.multiple_of(half * W, W), W)]
            return pltpu.make_async_copy(src, w_s.at[j % 2], w_sem.at[j % 2])
        raise ValueError

    def away(n):
        return (n == 0) | ((n >= 2) & (n <= 4))

    def group(n):
        return jnp.where(n < 2, 3, lax.rem(n + 1, 3))

    def qblock(n):
        at = pl.multiple_of(jnp.where(away(n), 1 - c, c) * 2048 + group(n) * W, W)
        return pltpu.make_async_copy(wq_hbm.at[:, pl.ds(at, W)], w_s.at[lax.rem(n, 2)], w_sem.at[lax.rem(n, 2)])

    def rcopy(src, dst, send, recv, device):
        return pltpu.make_async_remote_copy(src_ref=src, dst_ref=dst, send_sem=send, recv_sem=recv,
                                            device_id={"sp": device}, device_id_type=MESH)

    rows = T // 4
    xcopies = [pltpu.make_async_copy(x_hbm.at[pl.ds(r * rows, rows)], x_s.at[pl.ds(r * rows, rows)], x_sem.at[r]) for r in range(4)]
    for cp in xcopies:
        cp.start()
    near_copy = pltpu.make_async_copy(near_hbm, near_s, near_sem)
    near_copy.start()
    wblock(0).start()

    barrier = pltpu.get_barrier_semaphore()
    for d in (partner, straight, diagonal):
        pl.semaphore_signal(barrier, inc=1, device_id={"sp": d}, device_id_type=MESH)

    def norm(r, _):
        here = slice(r * 64, r * 64 + 64) if isinstance(r, int) else pl.ds(pl.multiple_of(r * 64, 64), 64)
        cols = [slice(n * HEAD, (n + 1) * HEAD) for n in range(D // HEAD)]
        total = jnp.zeros((64, HEAD), F32)
        for n in cols:
            wide = x_s[here, n].astype(F32)
            total += wide * wide
        scale = jnp.broadcast_to(lax.rsqrt(jnp.sum(total, -1, keepdims=True) * (1 / D) + 1e-6), (64, HEAD))
        for n in cols:
            a_s[here, n] = (x_s[here, n].astype(F32) * scale * gain_ref[n].astype(F32).reshape(1, HEAD)).astype(BF)

    for r in range(2):
        xcopies[r].wait()
        lax.fori_loop(r * rows // 64, (r + 1) * rows // 64, norm, None)
    xcopies[2].wait()
    xcopies[3].wait()
    wblock(1).start()

    near_copy.wait()
    c0, s0 = far_ref[pl.ds(me, 1), :], far_ref[pl.ds(me + 8, 1), :]
    left = lax.broadcasted_iota(jnp.int32, (T, HEAD), 1) < HEAD // 2
    table, swapped = near_s[...], pltpu.roll(near_s[...], HEAD // 2, 1)
    cos, sin = jnp.where(left, table, swapped), jnp.where(left, swapped, table)
    cos_s[...] = cos * c0 - sin * s0
    sin_s[...] = (sin * c0 + cos * s0) * jnp.where(left, -1.0, 1.0)

    def project(slot, out):
        z_s[out] = dot(a_s[...], w_s[slot], 1, 0).astype(BF)

    def turn(zslot, ref, lead):
        for h in range(4):
            z = z_s[zslot, :, h * HEAD:(h + 1) * HEAD].astype(F32)
            ref[(*lead, h)] = (z * cos_s[...] + pltpu.roll(z, HEAD // 2, 1) * sin_s[...]).astype(BF)

    def values(zslot, ref, lead):
        for h in range(4):
            ref[(*lead, h, slice(0, HEAD))] = z_s[zslot, :, h * HEAD:(h + 1) * HEAD].T

    for s in range(4):
        for h in range(4):
            v_s[s, h, HEAD:, :] = jnp.ones((16, T), BF)

    near_k = rcopy(k_s.at[4], k_s.at[c], kv_send.at[0], kv_recv.at[0], partner)
    near_v = rcopy(vt_s, v_s.at[c, :, pl.ds(0, HEAD)], kv_send.at[1], kv_recv.at[1], partner)

    def far(n, heads):
        to = (k_s.at[2 + c, heads], v_s.at[2 + c, heads, pl.ds(0, HEAD)])[n % 2]
        return rcopy((k_s.at[4, heads], vt_s.at[heads], k_s.at[c, heads], v_s.at[c, heads, pl.ds(0, HEAD)])[n], to,
                     far_send.at[n], far_recv.at[c, n % 2], diagonal if n < 2 else straight)

    def wait_far(s, heads):
        rcopy(k_s.at[4, heads], k_s.at[2 + s, heads], far_send.at[0], far_recv.at[s, 0], straight).wait_recv()
        rcopy(vt_s.at[heads], v_s.at[2 + s, heads, pl.ds(0, HEAD)], far_send.at[1], far_recv.at[s, 1], straight).wait_recv()

    three, fourth = pl.ds(0, 3), pl.ds(3, 1)

    def send_far(n):
        for which, heads in ((0, three), (1, fourth)):
            @pl.when(chip == which)
            def _():
                far(n, heads).start()

    wblock(0).wait()
    z_s[0, :T // 2] = dot(a_s[:T // 2], w_s[0], 1, 0).astype(BF)
    for r in range(T // 128, T // 64):
        norm(r, None)
    z_s[0, T // 2:] = dot(a_s[T // 2:], w_s[0], 1, 0).astype(BF)
    wblock(2).start()
    wblock(1).wait()
    pl.semaphore_wait(barrier, 3)
    project(1, 1)
    turn(0, k_s, (4,))
    wblock(3).start()
    near_k.start()
    send_far(0)
    wblock(2).wait()
    project(0, 0)
    values(1, vt_s, ())
    qblock(0).start()
    near_v.start()
    send_far(1)
    wblock(3).wait()
    project(1, 1)
    turn(0, k_s, (c,))
    qblock(1).start()
    send_far(2)
    qblock(0).wait()
    project(0, 0)
    values(1, v_s, (c,))
    qblock(2).start()
    send_far(3)

    def qcopy(i):
        return rcopy(q_s.at[2, i], q_s.at[c, i], q_send.at[i], q_recv.at[i], partner)

    def qfar(n, pair):
        two = pl.ds(2 * pair, 2)
        return rcopy(q_s.at[2, 3, two] if n == 0 else q_s.at[c, 3, two], qf_s.at[c, two], qf_send.at[n, pair], qf_recv.at[c, pair],
                     diagonal if n == 0 else straight)

    def queries(n, _):
        qblock(n).wait()
        turn(lax.rem(n + 1, 2), q_s, (jnp.where(away(n - 1), 2, c), group(n - 1)))
        project(lax.rem(n, 2), lax.rem(n, 2))

        @pl.when(n < 6)
        def _():
            qblock(n + 2).start()

        for at, copies in ((1, ((0, 0),)), (2, ((1, 0), (0, 1), (1, 1)))):
            @pl.when((n == at) & (chip == 1))
            def _():
                for m, pair in copies:
                    qfar(m, pair).start()

        @pl.when(away(n - 1))
        def _():
            qcopy(group(n - 1)).start()

    lax.fori_loop(1, 8, queries, None)
    turn(1, q_s, (c, 2))

    later = lax.broadcasted_iota(jnp.int32, (256, T), 1) % 256 >= lax.broadcasted_iota(jnp.int32, (256, T), 0)

    def attend(items, done=None, q_ref=None):
        n = len(items)
        scores, weights, keeps = {}, {}, {}
        cols = {"full": slice(0, T), "left": slice(0, 256), "right": slice(256, T)}
        keys = {"full": T, "left": 256, "right": T}

        def joined(parts, axis):
            return parts[0] if len(parts) == 1 else jnp.concatenate(parts, axis)

        def split(x, hs):
            wide = x.shape[-1] // len(hs)
            return [x[..., n * wide:(n + 1) * wide] for n in range(len(hs))]

        def qk(m):
            i, t, hs, s, _, kind = items[m]
            q = [q_s[t, i, h, cols[kind]] if q_ref is None else q_ref[t, h, cols[kind]] for h in hs]
            scores[m] = dot(k_s[s, i, 0:keys[kind]], joined(q, 0), 1, 1)

        def soft(m):
            i, t, hs, s, first, kind = items[m]
            x = scores.pop(m)
            if kind == "left":
                x = jnp.where(later, x, HIDDEN)
            if kind == "right":
                x = jnp.concatenate([x[:256], jnp.where(later, x[256:], HIDDEN)], 0)
            top = x.max(axis=0, keepdims=True)
            rows = [t * 16 + i * 4 + h for h in hs]
            if not first:
                old = joined([top_s[pl.ds(row, 1), cols[kind]] for row in rows], 1)
                top = jnp.maximum(old, top)
                keeps[m] = jnp.exp2((old - top) * E)
            for row, part in zip(rows, split(top, hs)):
                top_s[pl.ds(row, 1), cols[kind]] = part
            weights[m] = jnp.exp2((x - top) * E).astype(BF)

        def pv(m):
            i, t, hs, s, first, kind = items[m]
            new = split(dot(v_s[s, i, :, 0:keys[kind]], weights.pop(m), 1, 0)[:VR], hs)
            keep = [None] * len(hs) if first else split(keeps.pop(m), hs)
            for h, part, kept in zip(hs, new, keep):
                row = t * 16 + i * 4 + h
                if not first:
                    part = acc_s[row, :, cols[kind]] * kept + part
                if done is None or first:
                    acc_s[row, :, cols[kind]] = part
                else:
                    done(t, h, part)

        qk(0)
        qk(1)
        for m in range(n):
            soft(m)
            if m + 2 < n:
                qk(m + 2)
            if m >= 1:
                pv(m - 1)
        pv(n - 1)

    near_k.wait_recv()
    near_v.wait_recv()
    for i in range(4):
        qcopy(i).wait_recv()

    def local(i, _):
        pairs = ((0, 1), (2, 3))
        attend([(i, 0, hs, 0, True, side) for hs in pairs for side in ("left", "right")]
               + [(i, 1, (h,), 0, True, "full") for h in range(4)]
               + [(i, 1, hs, 1, False, side) for hs in pairs for side in ("left", "right")])

    def visits(pair):
        def visit(t, h):
            at = pl.multiple_of(c * 2048 + 3 * W + (2 * pair + h) * HEAD, HEAD)
            return rcopy(f_s.at[pair, 2 * t + h], seen_hbm.at[:, pl.ds(at, HEAD)], f_send.at[pair, 2 * t + h],
                         f_recv.at[c, 2 * pair + h], 2 + t)

        return [visit(t, h) for t in range(2) for h in range(2)]

    def visiting(pair, _):
        for s in range(2):
            rcopy(q_s.at[2, 3, pl.ds(0, 2)], qf_s.at[s, pl.ds(0, 2)], qf_send.at[0, 0], qf_recv.at[s, pair], straight).wait_recv()

        def done(t, h, total):
            f_s[pair, 2 * t + h - 2 * pair] = (total[:HEAD] * (1 / total[HEAD:HEAD + 1])).T.astype(BF)

        hs = (2 * pair, 2 * pair + 1)
        own = [(3, t, hs, 2 + t, True, side) for t in range(2) for side in ("left", "right")]
        attend(own + [(3, 1, (h,), 2, False, "full") for h in hs] + [(3, t, (h,), 0, False, "full") for t in range(2) for h in hs], None, qf_s)
        attend([(3, t, (h,), 1, False, "full") for t in range(2) for h in hs], done, qf_s)
        for cp in visits(pair):
            cp.start()

    @pl.when(chip == 0)
    def _():
        for s in range(2):
            wait_far(s, fourth)

        def both(pair, _):
            visiting(pair, None)
            lax.fori_loop(2 * pair, 2 * pair + 2, local, None)

        lax.fori_loop(0, 2, both, None)

    @pl.when(chip == 1)
    def _():
        lax.fori_loop(0, 3, local, None)

    def out_copies(i):
        par = lax.rem(i, 2)
        at = pl.multiple_of(c * 2048 + i * W, W)
        return [(rcopy(o_s2(par, 1 - c, h), seen_hbm.at[:, pl.ds(pl.multiple_of(at + h * HEAD, HEAD), HEAD)],
                       out_send.at[par, h], out_recv.at[i, h], partner),
                 pltpu.make_async_copy(o_s2(par, c, h), seen_hbm.at[:, pl.ds(pl.multiple_of(at + h * HEAD, HEAD), HEAD)],
                                       o_sem.at[par, h])) for h in range(4)]

    def o_s2(par, t, h):
        return o_s.at[par * 2 + t, h]

    def leave(count):
        for i in (count - 2, count - 1):
            for gone, home in out_copies(i):
                gone.wait_send()
                home.wait()
        for i in range(count):
            for gone, _ in out_copies(i):
                gone.wait_recv()

    def emit(i, work):
        par = lax.rem(i, 2)

        @pl.when(i >= 2)
        def _():
            for gone, home in out_copies(i - 2):
                gone.wait_send()
                home.wait()

        work(i, lambda t, h, total: o_s.__setitem__((par * 2 + t, h), (total[:HEAD] * (1 / total[HEAD:HEAD + 1])).T.astype(BF)))
        for gone, home in out_copies(i):
            gone.start()
            home.start()

    @pl.when(chip == 1)
    def _():
        wait_far(1 - c, three)

        def other(t, _):
            attend([(i, t, (h,), 3 - c, False, "full") for i in range(3) for h in range(4)])

        lax.fori_loop(0, 2, other, None)
        wait_far(c, three)

        def last(i, _):
            emit(i, lambda i, put: attend([(i, t, (h,), 2 + c, False, "full") for t in range(2) for h in range(4)], put))

        lax.fori_loop(0, 3, last, None)
        for n in range(4):
            far(n, fourth).wait_send()
        for m in range(2):
            for pair in range(2):
                qfar(m, pair).wait_send()
        leave(3)
        for half in range(2):
            for h in range(4):
                rcopy(f_s.at[0, 0], seen_hbm.at[:, pl.ds(0, HEAD)], f_send.at[0, 0], f_recv.at[half, h], straight).wait_recv()

    @pl.when(chip == 0)
    def _():
        def last(i, _):
            def work(i, put):
                for t in range(2):
                    for h in range(4):
                        put(t, h, acc_s[t * 16 + i * 4 + h])

            emit(i, work)

        lax.fori_loop(0, 4, last, None)
        for n in range(4):
            far(n, three).wait_send()
        for pair in range(2):
            for cp in visits(pair):
                cp.wait_send()
        leave(4)

    near_k.wait_send()
    near_v.wait_send()
    for i in range(4):
        qcopy(i).wait_send()


def attention(x, gain, wq, wk, wv):
    near, far = tables()
    hbm, vmem = pl.BlockSpec(memory_space=pl.ANY), pl.BlockSpec(memory_space=pltpu.VMEM)
    dma = pltpu.SemaphoreType.DMA
    return pl.pallas_call(
        fused,
        out_shape=jax.ShapeDtypeStruct((T, 4096), BF),
        in_specs=[hbm, vmem, hbm, vmem, hbm, hbm, hbm],
        out_specs=hbm,
        scratch_shapes=[
            pltpu.VMEM((T, D), BF), pltpu.VMEM((T, D), BF), pltpu.VMEM((2, D, W), BF), pltpu.VMEM((2, T, W), BF),
            pltpu.VMEM((T, HEAD), F32), pltpu.VMEM((T, HEAD), F32), pltpu.VMEM((T, HEAD), F32),
            pltpu.VMEM((3, 4, 4, T, HEAD), BF), pltpu.VMEM((5, 4, T, HEAD), BF), pltpu.VMEM((4, 4, HEAD + 16, T), BF),
            pltpu.VMEM((4, HEAD, T), BF), pltpu.VMEM((4, 4, T, HEAD), BF),
            pltpu.VMEM((32, T), F32), pltpu.VMEM((32, VR, T), F32),
            pltpu.VMEM((2, 4, T, HEAD), BF), pltpu.VMEM((2, 4, T, HEAD), BF),
            dma((4,)), dma, dma((2,)), dma((2, 4)),
            dma((2,)), dma((2,)), dma((4,)), dma((2, 2)), dma((4,)), dma((4,)), dma((2, 4)), dma((4, 4)),
            dma((2, 2)), dma((2, 2)), dma((2, 4)), dma((2, 4)),
        ],
        compiler_params=pltpu.CompilerParams(collective_id=0, has_side_effects=True, vmem_limit_bytes=63 * 2**20),
        cost_estimate=pl.CostEstimate(flops=45 * 10**9, bytes_accessed=80 * 10**6, transcendentals=30 * 10**6),
        name="project_attend",
    )(x, gain, jnp.asarray(near), jnp.asarray(far), wq, wk, wv)


def out_kernel(seen_hbm, w_hbm, x_hbm, y_hbm, s_s, w_s, x_s, z_s, y_s, first_sem, w_sem, x_sem, y_sem):
    k, blocks, slots = s_s.shape[1], D // W, 3
    parts = [(0, k // 8), (k // 8, k // 4), (3 * k // 8, k // 4), (5 * k // 8, 3 * k // 8)]
    pieces = []
    for n, (at, deep) in enumerate(parts):
        here = pl.ds(at, deep)
        pieces += [pltpu.make_async_copy(seen_hbm.at[:, here], s_s.at[:, here], first_sem.at[0, n]),
                   pltpu.make_async_copy(w_hbm.at[here, pl.ds(0, W)], w_s.at[0, here], first_sem.at[1, n])]

    def weights(j):
        at = pl.multiple_of(j * W, W)
        return pltpu.make_async_copy(w_hbm.at[:, pl.ds(at, W)], w_s.at[lax.rem(j, slots)], w_sem.at[lax.rem(j, slots)])

    def result(j):
        at = pl.multiple_of(j * W, W)
        return pltpu.make_async_copy(y_s.at[lax.rem(j, 2)], y_hbm.at[:, pl.ds(at, W)], y_sem.at[lax.rem(j, 2)])

    def finish(j):
        y_s[lax.rem(j, 2)] = (x_s[lax.rem(j, 3)].astype(F32) + z_s[lax.rem(j, 2)]).astype(BF)

    def residual(j):
        here = pl.ds(pl.multiple_of(j * W, W), W)
        return pltpu.make_async_copy(x_hbm.at[:, here], x_s.at[lax.rem(j, 3)], x_sem.at[lax.rem(j, 3)])

    for cp in pieces:
        cp.start()
    for n, (at, deep) in enumerate(parts):
        pieces[2 * n].wait()
        pieces[2 * n + 1].wait()
        if n == 2:
            weights(1).start()
            residual(0).start()
        here = slice(at, at + deep)
        part = dot(s_s[:, here], w_s[0, here], 1, 0)
        z_s[0] = part if n == 0 else z_s[0] + part
    residual(1).start()
    weights(2).start()

    def block(j, _):
        weights(j).wait()
        residual(j - 1).wait()
        finish(j - 1)
        z_s[lax.rem(j, 2)] = dot(s_s[...], w_s[lax.rem(j, slots)], 1, 0)

        @pl.when(j + 2 < blocks)
        def _():
            weights(j + 2).start()

        @pl.when(j + 1 < blocks)
        def _():
            residual(j + 1).start()

        result(j - 1).start()

        @pl.when(j >= 2)
        def _():
            result(j - 2).wait()

    lax.fori_loop(1, blocks, block, None)
    residual(blocks - 1).wait()
    finish(blocks - 1)
    result(blocks - 1).start()
    result(blocks - 2).wait()
    result(blocks - 1).wait()


def out_project(seen, wo, x):
    k = seen.shape[1]
    hbm, dma = pl.BlockSpec(memory_space=pl.ANY), pltpu.SemaphoreType.DMA
    return pl.pallas_call(
        out_kernel,
        out_shape=jax.ShapeDtypeStruct((T, D), BF),
        in_specs=[hbm] * 3,
        out_specs=hbm,
        scratch_shapes=[pltpu.VMEM((T, k), BF), pltpu.VMEM((3, k, W), BF), pltpu.VMEM((3, T, W), BF), pltpu.VMEM((2, T, W), F32),
                        pltpu.VMEM((2, T, W), BF), dma((2, 4)), dma((3,)), dma((3,)), dma((2,))],
        compiler_params=pltpu.CompilerParams(vmem_limit_bytes=60 * 2**20),
        cost_estimate=pl.CostEstimate(flops=2 * T * k * D, bytes_accessed=2 * (k * D + T * k + 2 * T * D), transcendentals=0),
        name="out_project",
    )(seen, wo, x)


def solution(mesh):
    def step(x, gain, wq, wk, wv, wo):
        return out_project(attention(x, gain, wq, wk, wv), wo, x)

    tokens, whole = P(("dp", "sp"), None), P(None, None)
    return jax.shard_map(step, mesh=mesh, in_specs=(tokens, P(None), whole, whole, whole, whole), out_specs=tokens, check_vma=False)
```

```python
import functools

import jax
import jax.numpy as jnp
import numpy as np
from jax import lax
from jax.experimental import pallas as pl
from jax.experimental.pallas import tpu as pltpu
from jax.sharding import PartitionSpec as P

MESH = pl.DeviceIdType.MESH
NEG = -1e30
HIDDEN = 2 * NEG
HEAD = 128
THETA = 10000
T = 512
D = 5120
W = 512
E = HEAD**-0.5 * 1.4426950408889634
VR = 136
BF, F32 = jnp.bfloat16, jnp.float32


def dot(a, b, ca, cb):
    return lax.dot_general(a, b, (((ca,), (cb,)), ((), ())), preferred_element_type=F32)


def tables():
    half = HEAD // 2
    freq = np.float64(THETA) ** (-np.arange(half) / half)
    near, far = np.arange(T)[:, None] * freq, (np.arange(8) * T)[:, None] * freq
    far = np.concatenate([far, far], 1)
    return [t.astype(np.float32) for t in (np.concatenate([np.cos(near), np.sin(near)], 1), np.concatenate([np.cos(far), np.sin(far)]))]


def fused(x_hbm, gain_ref, near_hbm, far_ref, wq_hbm, wk_hbm, wv_hbm, seen_hbm,
          x_s, a_s, w_s, z_s, near_s, cos_s, sin_s, q_s, k_s, v_s, vt_s, o_s, top_s, acc_s, qf_s, f_s,
          x_sem, near_sem, w_sem, o_sem, kv_send, kv_recv, far_send, far_recv, q_send, q_recv, out_send, out_recv,
          qf_send, qf_recv, f_send, f_recv):
    me = lax.axis_index("sp")
    c, chip = lax.rem(me, 2), lax.div(me, 2)
    partner = me + 1 - 2 * c
    straight = lax.rem(me + 2, 4)
    diagonal = lax.rem(partner + 2, 4)

    def wblock(j):
        if j < 4:
            half = 1 - c if j < 2 else c
            src = (wk_hbm if j % 2 == 0 else wv_hbm).at[:, pl.ds(pl.multiple_of(half * W, W), W)]
            return pltpu.make_async_copy(src, w_s.at[j % 2], w_sem.at[j % 2])
        raise ValueError

    def away(n):
        return (n == 0) | ((n >= 2) & (n <= 4))

    def group(n):
        return jnp.where(n < 2, 3, lax.rem(n + 1, 3))

    def qblock(n):
        at = pl.multiple_of(jnp.where(away(n), 1 - c, c) * 2048 + group(n) * W, W)
        return pltpu.make_async_copy(wq_hbm.at[:, pl.ds(at, W)], w_s.at[lax.rem(n, 2)], w_sem.at[lax.rem(n, 2)])

    def rcopy(src, dst, send, recv, device):
        return pltpu.make_async_remote_copy(src_ref=src, dst_ref=dst, send_sem=send, recv_sem=recv,
                                            device_id={"sp": device}, device_id_type=MESH)

    rows = T // 4
    xcopies = [pltpu.make_async_copy(x_hbm.at[pl.ds(r * rows, rows)], x_s.at[pl.ds(r * rows, rows)], x_sem.at[r]) for r in range(4)]
    for cp in xcopies:
        cp.start()
    deep = D // 2
    first = [pltpu.make_async_copy(wk_hbm.at[pl.ds(n * deep, deep), pl.ds(pl.multiple_of((1 - c) * W, W), W)],
                                   w_s.at[0, pl.ds(n * deep, deep)], w_sem.at[2 * n]) for n in range(2)]
    near_copy = pltpu.make_async_copy(near_hbm, near_s, near_sem)
    for cp in (*first, near_copy):
        cp.start()

    barrier = pltpu.get_barrier_semaphore()
    for d in (partner, straight, diagonal):
        pl.semaphore_signal(barrier, inc=1, device_id={"sp": d}, device_id_type=MESH)

    def norm(r, _):
        here = slice(r * 64, r * 64 + 64) if isinstance(r, int) else pl.ds(pl.multiple_of(r * 64, 64), 64)
        cols = [slice(n * HEAD, (n + 1) * HEAD) for n in range(D // HEAD)]
        total = jnp.zeros((64, HEAD), F32)
        for n in cols:
            wide = x_s[here, n].astype(F32)
            total += wide * wide
        scale = jnp.broadcast_to(lax.rsqrt(jnp.sum(total, -1, keepdims=True) * (1 / D) + 1e-6), (64, HEAD))
        for n in cols:
            a_s[here, n] = (x_s[here, n].astype(F32) * scale * gain_ref[n].astype(F32).reshape(1, HEAD)).astype(BF)

    for r in range(2):
        xcopies[r].wait()
        lax.fori_loop(r * rows // 64, (r + 1) * rows // 64, norm, None)
    xcopies[2].wait()
    xcopies[3].wait()
    wblock(1).start()

    def project(slot, out):
        z_s[out] = dot(a_s[...], w_s[slot], 1, 0).astype(BF)

    def turn(zslot, ref, lead):
        for h in range(4):
            z = z_s[zslot, :, h * HEAD:(h + 1) * HEAD].astype(F32)
            ref[(*lead, h)] = (z * cos_s[...] + pltpu.roll(z, HEAD // 2, 1) * sin_s[...]).astype(BF)

    def values(zslot, ref, lead):
        for h in range(4):
            ref[(*lead, h, slice(0, HEAD))] = z_s[zslot, :, h * HEAD:(h + 1) * HEAD].T

    for s in range(4):
        for h in range(4):
            v_s[s, h, HEAD:, :] = jnp.ones((16, T), BF)

    near_k = rcopy(k_s.at[4], k_s.at[c], kv_send.at[0], kv_recv.at[0], partner)
    near_v = rcopy(vt_s, v_s.at[c, :, pl.ds(0, HEAD)], kv_send.at[1], kv_recv.at[1], partner)

    def far(n, heads):
        to = (k_s.at[2 + c, heads], v_s.at[2 + c, heads, pl.ds(0, HEAD)])[n % 2]
        return rcopy((k_s.at[4, heads], vt_s.at[heads], k_s.at[c, heads], v_s.at[c, heads, pl.ds(0, HEAD)])[n], to,
                     far_send.at[n], far_recv.at[c, n % 2], diagonal if n < 2 else straight)

    def wait_far(s, heads):
        rcopy(k_s.at[4, heads], k_s.at[2 + s, heads], far_send.at[0], far_recv.at[s, 0], straight).wait_recv()
        rcopy(vt_s.at[heads], v_s.at[2 + s, heads, pl.ds(0, HEAD)], far_send.at[1], far_recv.at[s, 1], straight).wait_recv()

    three, fourth = pl.ds(0, 3), pl.ds(3, 1)

    def send_far(n):
        for which, heads in ((0, three), (1, fourth)):
            @pl.when(chip == which)
            def _():
                far(n, heads).start()

    first[0].wait()
    acc_s[0:2, :HEAD, :] = dot(a_s[:T // 2, :deep], w_s[0, :deep], 1, 0).reshape(2, HEAD, W)
    first[1].wait()
    part = acc_s[0:2, :HEAD, :].reshape(T // 2, W) + dot(a_s[:T // 2, deep:], w_s[0, deep:], 1, 0)
    z_s[0, :T // 2] = part.astype(BF)
    for r in range(T // 128, T // 64):
        norm(r, None)
    z_s[0, T // 2:] = dot(a_s[T // 2:], w_s[0], 1, 0).astype(BF)
    wblock(2).start()

    near_copy.wait()
    c0, s0 = far_ref[pl.ds(me, 1), :], far_ref[pl.ds(me + 8, 1), :]
    left = lax.broadcasted_iota(jnp.int32, (T, HEAD), 1) < HEAD // 2
    table, swapped = near_s[...], pltpu.roll(near_s[...], HEAD // 2, 1)
    cos, sin = jnp.where(left, table, swapped), jnp.where(left, swapped, table)
    cos_s[...] = cos * c0 - sin * s0
    sin_s[...] = (sin * c0 + cos * s0) * jnp.where(left, -1.0, 1.0)

    wblock(1).wait()
    pl.semaphore_wait(barrier, 3)
    project(1, 1)
    turn(0, k_s, (4,))
    wblock(3).start()
    near_k.start()
    send_far(0)
    wblock(2).wait()
    project(0, 0)
    values(1, vt_s, ())
    qblock(0).start()
    near_v.start()
    send_far(1)
    wblock(3).wait()
    project(1, 1)
    turn(0, k_s, (c,))
    qblock(1).start()
    send_far(2)
    qblock(0).wait()
    project(0, 0)
    values(1, v_s, (c,))
    qblock(2).start()
    send_far(3)

    def qcopy(i):
        return rcopy(q_s.at[2, i], q_s.at[c, i], q_send.at[i], q_recv.at[i], partner)

    def qfar(n, pair):
        two = pl.ds(2 * pair, 2)
        return rcopy(q_s.at[2, 3, two] if n == 0 else q_s.at[c, 3, two], qf_s.at[c, two], qf_send.at[n, pair], qf_recv.at[c, pair],
                     diagonal if n == 0 else straight)

    def queries(n, _):
        qblock(n).wait()
        turn(lax.rem(n + 1, 2), q_s, (jnp.where(away(n - 1), 2, c), group(n - 1)))
        project(lax.rem(n, 2), lax.rem(n, 2))

        @pl.when(n < 6)
        def _():
            qblock(n + 2).start()

        for at, copies in ((1, ((0, 0),)), (2, ((1, 0), (0, 1), (1, 1)))):
            @pl.when((n == at) & (chip == 1))
            def _():
                for m, pair in copies:
                    qfar(m, pair).start()

        @pl.when(away(n - 1))
        def _():
            qcopy(group(n - 1)).start()

    lax.fori_loop(1, 8, queries, None)
    turn(1, q_s, (c, 2))

    later = lax.broadcasted_iota(jnp.int32, (256, T), 1) % 256 >= lax.broadcasted_iota(jnp.int32, (256, T), 0)

    def attend(items, done=None, q_ref=None):
        n = len(items)
        scores, weights, keeps = {}, {}, {}
        cols = {"full": slice(0, T), "left": slice(0, 256), "right": slice(256, T)}
        keys = {"full": T, "left": 256, "right": T}

        def joined(parts, axis):
            return parts[0] if len(parts) == 1 else jnp.concatenate(parts, axis)

        def split(x, hs):
            wide = x.shape[-1] // len(hs)
            return [x[..., n * wide:(n + 1) * wide] for n in range(len(hs))]

        def qk(m):
            i, t, hs, s, _, kind = items[m]
            q = [q_s[t, i, h, cols[kind]] if q_ref is None else q_ref[t, h, cols[kind]] for h in hs]
            scores[m] = dot(k_s[s, i, 0:keys[kind]], joined(q, 0), 1, 1)

        def soft(m):
            i, t, hs, s, first, kind = items[m]
            x = scores.pop(m)
            if kind == "left":
                x = jnp.where(later, x, HIDDEN)
            if kind == "right":
                x = jnp.concatenate([x[:256], jnp.where(later, x[256:], HIDDEN)], 0)
            top = x.max(axis=0, keepdims=True)
            rows = [t * 16 + i * 4 + h for h in hs]
            if not first:
                old = joined([top_s[pl.ds(row, 1), cols[kind]] for row in rows], 1)
                top = jnp.maximum(old, top)
                keeps[m] = jnp.exp2((old - top) * E)
            for row, part in zip(rows, split(top, hs)):
                top_s[pl.ds(row, 1), cols[kind]] = part
            weights[m] = jnp.exp2((x - top) * E).astype(BF)

        def pv(m):
            i, t, hs, s, first, kind = items[m]
            new = split(dot(v_s[s, i, :, 0:keys[kind]], weights.pop(m), 1, 0)[:VR], hs)
            keep = [None] * len(hs) if first else split(keeps.pop(m), hs)
            for h, part, kept in zip(hs, new, keep):
                row = t * 16 + i * 4 + h
                if not first:
                    part = acc_s[row, :, cols[kind]] * kept + part
                if done is None or first:
                    acc_s[row, :, cols[kind]] = part
                else:
                    done(t, h, part)

        qk(0)
        qk(1)
        for m in range(n):
            soft(m)
            if m + 2 < n:
                qk(m + 2)
            if m >= 1:
                pv(m - 1)
        pv(n - 1)

    near_k.wait_recv()
    near_v.wait_recv()
    for i in range(4):
        qcopy(i).wait_recv()

    def local(i, _):
        pairs = ((0, 1), (2, 3))
        attend([(i, 0, hs, 0, True, side) for hs in pairs for side in ("left", "right")]
               + [(i, 1, (h,), 0, True, "full") for h in range(4)]
               + [(i, 1, hs, 1, False, side) for hs in pairs for side in ("left", "right")])

    def visits(pair):
        def visit(t, h):
            at = pl.multiple_of(c * 2048 + 3 * W + (2 * pair + h) * HEAD, HEAD)
            return rcopy(f_s.at[pair, 2 * t + h], seen_hbm.at[:, pl.ds(at, HEAD)], f_send.at[pair, 2 * t + h],
                         f_recv.at[c, 2 * pair + h], 2 + t)

        return [visit(t, h) for t in range(2) for h in range(2)]

    def visiting(pair, _):
        for s in range(2):
            rcopy(q_s.at[2, 3, pl.ds(0, 2)], qf_s.at[s, pl.ds(0, 2)], qf_send.at[0, 0], qf_recv.at[s, pair], straight).wait_recv()

        def done(t, h, total):
            f_s[pair, 2 * t + h - 2 * pair] = (total[:HEAD] * (1 / total[HEAD:HEAD + 1])).T.astype(BF)

        hs = (2 * pair, 2 * pair + 1)
        own = [(3, t, hs, 2 + t, True, side) for t in range(2) for side in ("left", "right")]
        attend(own + [(3, 1, (h,), 2, False, "full") for h in hs] + [(3, t, (h,), 0, False, "full") for t in range(2) for h in hs], None, qf_s)
        attend([(3, t, (h,), 1, False, "full") for t in range(2) for h in hs], done, qf_s)
        for cp in visits(pair):
            cp.start()

    @pl.when(chip == 0)
    def _():
        for s in range(2):
            wait_far(s, fourth)

        def both(pair, _):
            visiting(pair, None)
            lax.fori_loop(2 * pair, 2 * pair + 2, local, None)

        lax.fori_loop(0, 2, both, None)

    @pl.when(chip == 1)
    def _():
        lax.fori_loop(0, 3, local, None)

    def out_copies(i):
        par = lax.rem(i, 2)
        at = pl.multiple_of(c * 2048 + i * W, W)
        return [(rcopy(o_s2(par, 1 - c, h), seen_hbm.at[:, pl.ds(pl.multiple_of(at + h * HEAD, HEAD), HEAD)],
                       out_send.at[par, h], out_recv.at[i, h], partner),
                 pltpu.make_async_copy(o_s2(par, c, h), seen_hbm.at[:, pl.ds(pl.multiple_of(at + h * HEAD, HEAD), HEAD)],
                                       o_sem.at[par, h])) for h in range(4)]

    def o_s2(par, t, h):
        return o_s.at[par * 2 + t, h]

    def leave(count):
        for i in (count - 2, count - 1):
            for gone, home in out_copies(i):
                gone.wait_send()
                home.wait()
        for i in range(count):
            for gone, _ in out_copies(i):
                gone.wait_recv()

    def emit(i, work):
        par = lax.rem(i, 2)

        @pl.when(i >= 2)
        def _():
            for gone, home in out_copies(i - 2):
                gone.wait_send()
                home.wait()

        work(i, lambda t, h, total: o_s.__setitem__((par * 2 + t, h), (total[:HEAD] * (1 / total[HEAD:HEAD + 1])).T.astype(BF)))
        for gone, home in out_copies(i):
            gone.start()
            home.start()

    @pl.when(chip == 1)
    def _():
        wait_far(1 - c, three)

        def other(t, _):
            attend([(i, t, (h,), 3 - c, False, "full") for i in range(3) for h in range(4)])

        lax.fori_loop(0, 2, other, None)
        wait_far(c, three)

        def last(i, _):
            emit(i, lambda i, put: attend([(i, t, (h,), 2 + c, False, "full") for t in range(2) for h in range(4)], put))

        lax.fori_loop(0, 3, last, None)
        for n in range(4):
            far(n, fourth).wait_send()
        for m in range(2):
            for pair in range(2):
                qfar(m, pair).wait_send()
        leave(3)
        for half in range(2):
            for h in range(4):
                rcopy(f_s.at[0, 0], seen_hbm.at[:, pl.ds(0, HEAD)], f_send.at[0, 0], f_recv.at[half, h], straight).wait_recv()

    @pl.when(chip == 0)
    def _():
        def last(i, _):
            def work(i, put):
                for t in range(2):
                    for h in range(4):
                        put(t, h, acc_s[t * 16 + i * 4 + h])

            emit(i, work)

        lax.fori_loop(0, 4, last, None)
        for n in range(4):
            far(n, three).wait_send()
        for pair in range(2):
            for cp in visits(pair):
                cp.wait_send()
        leave(4)

    near_k.wait_send()
    near_v.wait_send()
    for i in range(4):
        qcopy(i).wait_send()


def attention(x, gain, wq, wk, wv):
    near, far = tables()
    hbm, vmem = pl.BlockSpec(memory_space=pl.ANY), pl.BlockSpec(memory_space=pltpu.VMEM)
    dma = pltpu.SemaphoreType.DMA
    return pl.pallas_call(
        fused,
        out_shape=jax.ShapeDtypeStruct((T, 4096), BF),
        in_specs=[hbm, vmem, hbm, vmem, hbm, hbm, hbm],
        out_specs=hbm,
        scratch_shapes=[
            pltpu.VMEM((T, D), BF), pltpu.VMEM((T, D), BF), pltpu.VMEM((2, D, W), BF), pltpu.VMEM((2, T, W), BF),
            pltpu.VMEM((T, HEAD), F32), pltpu.VMEM((T, HEAD), F32), pltpu.VMEM((T, HEAD), F32),
            pltpu.VMEM((3, 4, 4, T, HEAD), BF), pltpu.VMEM((5, 4, T, HEAD), BF), pltpu.VMEM((4, 4, HEAD + 16, T), BF),
            pltpu.VMEM((4, HEAD, T), BF), pltpu.VMEM((4, 4, T, HEAD), BF),
            pltpu.VMEM((32, T), F32), pltpu.VMEM((32, VR, T), F32),
            pltpu.VMEM((2, 4, T, HEAD), BF), pltpu.VMEM((2, 4, T, HEAD), BF),
            dma((4,)), dma, dma((3,)), dma((2, 4)),
            dma((2,)), dma((2,)), dma((4,)), dma((2, 2)), dma((4,)), dma((4,)), dma((2, 4)), dma((4, 4)),
            dma((2, 2)), dma((2, 2)), dma((2, 4)), dma((2, 4)),
        ],
        compiler_params=pltpu.CompilerParams(collective_id=0, has_side_effects=True, vmem_limit_bytes=63 * 2**20),
        cost_estimate=pl.CostEstimate(flops=45 * 10**9, bytes_accessed=80 * 10**6, transcendentals=30 * 10**6),
        name="project_attend",
    )(x, gain, jnp.asarray(near), jnp.asarray(far), wq, wk, wv)


def out_kernel(seen_hbm, w_hbm, x_hbm, y_hbm, s_s, w_s, x_s, z_s, y_s, first_sem, w_sem, x_sem, y_sem):
    k, blocks, slots = s_s.shape[1], D // W, 3
    parts = [(0, k // 8), (k // 8, k // 4), (3 * k // 8, k // 4), (5 * k // 8, 3 * k // 8)]
    pieces = []
    for n, (at, deep) in enumerate(parts):
        here = pl.ds(at, deep)
        pieces += [pltpu.make_async_copy(seen_hbm.at[:, here], s_s.at[:, here], first_sem.at[0, n]),
                   pltpu.make_async_copy(w_hbm.at[here, pl.ds(0, W)], w_s.at[0, here], first_sem.at[1, n])]

    def weights(j):
        at = pl.multiple_of(j * W, W)
        return pltpu.make_async_copy(w_hbm.at[:, pl.ds(at, W)], w_s.at[lax.rem(j, slots)], w_sem.at[lax.rem(j, slots)])

    def result(j):
        at = pl.multiple_of(j * W, W)
        return pltpu.make_async_copy(y_s.at[lax.rem(j, 2)], y_hbm.at[:, pl.ds(at, W)], y_sem.at[lax.rem(j, 2)])

    def finish(j):
        y_s[lax.rem(j, 2)] = (x_s[lax.rem(j, 3)].astype(F32) + z_s[lax.rem(j, 2)]).astype(BF)

    def residual(j):
        here = pl.ds(pl.multiple_of(j * W, W), W)
        return pltpu.make_async_copy(x_hbm.at[:, here], x_s.at[lax.rem(j, 3)], x_sem.at[lax.rem(j, 3)])

    for cp in pieces:
        cp.start()
    for n, (at, deep) in enumerate(parts):
        pieces[2 * n].wait()
        pieces[2 * n + 1].wait()
        if n == 2:
            weights(1).start()
            residual(0).start()
        here = slice(at, at + deep)
        part = dot(s_s[:, here], w_s[0, here], 1, 0)
        z_s[0] = part if n == 0 else z_s[0] + part
    residual(1).start()
    weights(2).start()

    def block(j, _):
        weights(j).wait()
        residual(j - 1).wait()
        finish(j - 1)
        z_s[lax.rem(j, 2)] = dot(s_s[...], w_s[lax.rem(j, slots)], 1, 0)

        @pl.when(j + 2 < blocks)
        def _():
            weights(j + 2).start()

        @pl.when(j + 1 < blocks)
        def _():
            residual(j + 1).start()

        result(j - 1).start()

        @pl.when(j >= 2)
        def _():
            result(j - 2).wait()

    lax.fori_loop(1, blocks, block, None)
    residual(blocks - 1).wait()
    finish(blocks - 1)
    result(blocks - 1).start()
    result(blocks - 2).wait()
    result(blocks - 1).wait()


def out_project(seen, wo, x):
    k = seen.shape[1]
    hbm, dma = pl.BlockSpec(memory_space=pl.ANY), pltpu.SemaphoreType.DMA
    return pl.pallas_call(
        out_kernel,
        out_shape=jax.ShapeDtypeStruct((T, D), BF),
        in_specs=[hbm] * 3,
        out_specs=hbm,
        scratch_shapes=[pltpu.VMEM((T, k), BF), pltpu.VMEM((3, k, W), BF), pltpu.VMEM((3, T, W), BF), pltpu.VMEM((2, T, W), F32),
                        pltpu.VMEM((2, T, W), BF), dma((2, 4)), dma((3,)), dma((3,)), dma((2,))],
        compiler_params=pltpu.CompilerParams(vmem_limit_bytes=60 * 2**20),
        cost_estimate=pl.CostEstimate(flops=2 * T * k * D, bytes_accessed=2 * (k * D + T * k + 2 * T * D), transcendentals=0),
        name="out_project",
    )(seen, wo, x)


def solution(mesh):
    def step(x, gain, wq, wk, wv, wo):
        return out_project(attention(x, gain, wq, wk, wv), wo, x)

    tokens, whole = P(("dp", "sp"), None), P(None, None)
    return jax.shard_map(step, mesh=mesh, in_specs=(tokens, P(None), whole, whole, whole, whole), out_specs=tokens, check_vma=False)
```
